32 devices in a mesh: gx: 8 (over z, y), gy: 4 (over x, core).
Axes of the slice: x: 2, y: 2, z: 4, core: 2. Of those that a mesh axis runs over, the one named last changes fastest.
Arguments:
- image_feats: bfloat16 [16384, 4096], P('gx', 'gy'), may hold values from -6 to 6
- w_kv: bfloat16 [4096, 2048], P('gy'), may hold values from -0.09375 to 0.09375
- k_gain: float32 [128], replicated, may hold values from 0.25 to 1.75
- tile_rows: int32 [128], replicated, may hold values from 0 to 128
- deal: int32 [8, 16], replicated, may hold values from 0 to 127, as said below
Outputs:
- keys_out: bfloat16 [16384, 1024], P('gx', 'gy')
- values_out: bfloat16 [16384, 1024], P('gx', 'gy')
The draws below stay inside these ranges and needn't reach their ends.
Inputs may be any that keep to these rules, and one draw needn't show every extreme that they name: Each input tile is named exactly once; deal[j, s] % 16 == s; two entries of one row j that name tiles of the same index of gx stand in columns s that differ by a multiple of 8, so one row names at most 2 tiles of one index of gx, and exactly 2 for some.
All inputs are finite; a program needn't handle non-finite values.
Results may differ from the reference program's by a relative error of at most 0.001.
Values may be sent and summed in bfloat16 or wider, within the bound.
A program may use at most 128 MiB of HBM per device.

```python
import jax
import jax.numpy as jnp
from jax import lax

D = 4096
HEADS = 8
HD = 128
TILE = 128
TPD = 16
KV = 1024
TILES = 128
ROWS = 16384
N_GX = 8


def draw_deal(key, part):
    inner = jax.random.fold_in(key, 7)
    first_key, second_key = jax.random.split(inner)
    base = jax.random.permutation(first_key, N_GX)
    shuffled = jax.random.permutation(second_key, N_GX)
    slot_index = jnp.arange(TPD, dtype=jnp.int32)
    offsets = shuffled[slot_index % N_GX]
    column = jnp.arange(N_GX, dtype=jnp.int32)[:, None]
    source_device = base[(column + offsets[None, :]) % N_GX]
    return (source_device * TPD + slot_index[None, :]).astype(jnp.int32)


def with_ends(drawn, own_key, least, top_value):
    dims = drawn.shape
    spot = [jax.random.randint(jax.random.fold_in(own_key, axis), (), 0, dims[axis]) for axis in range(len(dims))]
    drawn = drawn.at[tuple(spot)].set(least)
    longest = dims.index(max(dims))
    spot[longest] = (spot[longest] + 1) % dims[longest]
    return drawn.at[tuple(spot)].set(top_value)


def shard_levels(own_key, shape, cuts, smallest, top_value):
    loudness, own = 1.0, jax.random.fold_in(own_key, 6)
    for dim, blocks in cuts:
        steps = jnp.exp(jax.random.uniform(jax.random.fold_in(own, dim), (blocks,), jnp.float32, smallest / len(cuts), top_value / len(cuts)))
        loudness = loudness * jnp.repeat(steps, shape[dim] // blocks).reshape([-1 if axis == dim else 1 for axis in range(len(shape))])
    return loudness


def scatter_about(stream_key, dims, deviation, reach, shards=(), kind=jnp.bfloat16):
    gain = shard_levels(stream_key, dims, shards, -0.22, 0.18) if shards else 1.0
    result = jax.random.normal(stream_key, dims, jnp.float32) * deviation * gain
    return jnp.minimum(jnp.maximum(result, -reach), reach).astype(kind)


def setup_inputs(seed: int = 0) -> dict:
    keys = jax.random.split(jax.random.key(seed), 6)
    image_feats = scatter_about(keys[0], (ROWS, D), 1.0, 6.0, ((0, 8), (1, 4)))
    w_kv = scatter_about(keys[1], (D, 2 * KV), D ** -0.5, 0.09375, ((0, 4),))
    k_gain = jnp.clip(1.0 + 0.15 * jax.random.normal(keys[2], (HD,), jnp.float32), 0.25, 1.75)
    tile_rows = with_ends(jax.random.randint(keys[3], (TILES,), 0, TILE + 1), jax.random.fold_in(keys[3], 1), 0, TILE).astype(jnp.int32)
    deal = draw_deal(jax.random.fold_in(keys[5], 71), 0)
    return {"image_feats": image_feats, "w_kv": w_kv, "k_gain": k_gain, "tile_rows": tile_rows, "deal": deal}


epsilon = 1e-05

def reference(image_feats, w_kv, k_gain, tile_rows, deal):
    tiled = image_feats.reshape(TILES, TILE, D)
    order = deal.reshape(-1).astype(jnp.int32)
    dealt = jnp.take(tiled, order, axis=0).reshape(ROWS, D)
    projected = jnp.dot(dealt, w_kv, preferred_element_type=jnp.float32)
    projected = projected.reshape(ROWS, 2, HEADS, HD)
    key_pre = projected[:, 0]
    value_pre = projected[:, 1]
    mean_square = lax.optimization_barrier(jnp.mean(key_pre * key_pre, axis=-1, keepdims=True))
    normed = key_pre * lax.rsqrt(mean_square + epsilon) * k_gain
    limits = jnp.take(tile_rows, order, axis=0)
    position = jnp.arange(TILE, dtype=jnp.int32)
    valid = (position[None, :] < limits[:, None]).reshape(ROWS, 1, 1)
    keys_out = jnp.where(valid, normed, 0.0).reshape(ROWS, KV).astype(jnp.bfloat16)
    values_out = jnp.where(valid, value_pre, 0.0).reshape(ROWS, KV).astype(jnp.bfloat16)
    return (keys_out, values_out)
```

```python
import functools

import jax
import jax.numpy as jnp
from jax import lax
from jax.experimental import pallas as pl
from jax.experimental.pallas import tpu as pltpu
from jax.sharding import PartitionSpec as P

HD = 128
TILE = 128
TPD = 16


epsilon = 1e-05


def plain_local(image_feats, w_kv, k_gain, tile_rows, deal):
    local_width = image_feats.shape[1]
    groups = lax.axis_size("gx")
    own_index = lax.axis_index("gx")
    slots = max(1, TPD // groups)
    wanted = lax.dynamic_index_in_dim(deal, own_index, 0, keepdims=False)
    slot_index = jnp.arange(TPD, dtype=jnp.int32)
    slot_class = slot_index // groups
    places = jnp.arange(slots, dtype=jnp.int32)
    class_match = slot_class[None, :] == places[:, None]
    own_tiles = own_index * TPD + slot_index
    sending = deal == own_tiles[None, :]
    send_select = (sending[:, None, :] & class_match[None, :, :]).astype(jnp.bfloat16)
    blocks = image_feats.reshape(TPD, TILE, local_width)
    outgoing = jnp.einsum(
        "dcs,str->dctr", send_select, blocks, preferred_element_type=jnp.float32
    ).astype(jnp.bfloat16)
    incoming = lax.all_to_all(outgoing, "gx", split_axis=0, concat_axis=0, tiled=True)
    sources = jnp.arange(groups, dtype=jnp.int32)
    from_source = (wanted // TPD)[:, None] == sources[None, :]
    take_select = (from_source[:, :, None] & class_match.T[:, None, :]).astype(jnp.bfloat16)
    dealt_tiles = jnp.einsum(
        "snc,nctr->str", take_select, incoming, preferred_element_type=jnp.float32
    ).astype(jnp.bfloat16)
    row_count = TPD * TILE
    dealt_rows = dealt_tiles.reshape(row_count, local_width)
    total_kv = w_kv.shape[1] // 2
    partial_value = jnp.dot(dealt_rows, w_kv, preferred_element_type=jnp.float32)
    projected = lax.psum_scatter(
        partial_value.reshape(row_count, 2, total_kv), "gy", scatter_dimension=2, tiled=True
    )
    share_cols = projected.shape[2]
    key_pre = projected[:, 0, :].reshape(row_count, share_cols // HD, HD)
    value_pre = projected[:, 1, :]
    mean_square = jnp.mean(key_pre * key_pre, axis=-1, keepdims=True)
    normed = (key_pre * lax.rsqrt(mean_square + epsilon) * k_gain).reshape(row_count, share_cols)
    all_tiles = jnp.arange(tile_rows.shape[0], dtype=jnp.int32)
    limits = jnp.sum(
        jnp.where(wanted[:, None] == all_tiles[None, :], tile_rows[None, :], 0), axis=1
    )
    position = jnp.arange(TILE, dtype=jnp.int32)
    valid_rows = (position[None, :] < limits[:, None]).reshape(row_count, 1)
    keys_out = jnp.where(valid_rows, normed, 0.0).astype(jnp.bfloat16)
    values_out = jnp.where(valid_rows, value_pre, 0.0).astype(jnp.bfloat16)
    return (keys_out, values_out)


MESH = pl.DeviceIdType.MESH
PIECE = 16
SCALES = 8
STEPS = 32767.0
LEAST = 1e-30
LEAD = 3


def route(step, me, groups, slots):
    flips = groups - 1 - step // slots
    target, bit = 0, 1
    while bit < groups:
        target += (me // bit + flips // bit) % 2 * bit
        bit *= 2
    return target, step % slots


def tables(me, groups, slots, tile_rows, deal):
    per_tile = TILE // PIECE
    step = jnp.arange(TPD, dtype=jnp.int32)
    target, cls = route(step, me, groups, slots)
    column = jnp.arange(TPD, dtype=jnp.int32)
    row = jnp.arange(groups, dtype=jnp.int32)
    named = deal == (me * TPD + column)[None, :]
    chosen = (
        named[None] & (target[:, None] == row)[:, :, None]
        & (cls[:, None] == column // groups)[:, None, :]
    )
    slot = jnp.sum(jnp.where(chosen, column, 0), axis=(1, 2))
    own_rows = lax.dynamic_slice(tile_rows, (me * TPD,), (TPD,))
    limit = jnp.sum(jnp.where(slot[:, None] == column[None, :], own_rows[None, :], 0), axis=1)
    count = jnp.maximum((limit + PIECE - 1) // PIECE, 1)
    first = jnp.sum(jnp.where(step[None, :] < step[:, None], count[None, :], 0), axis=1)
    place = jnp.arange(TPD * per_tile, dtype=jnp.int32)[:, None]
    inside = (first[None, :] <= place) & (place < (first + count)[None, :])
    source = jnp.sum(
        jnp.where(inside, slot[None, :] * per_tile + place - first[None, :], 0), axis=1
    )
    part = jnp.arange(per_tile, dtype=jnp.int32)[None, :]
    piece = first[:, None] + jnp.minimum(part, count[:, None] - 1)
    return source, piece.reshape(-1), limit


def project_kernel(
    groups, slots, chunks, source_ref, piece_ref, limit_ref, gain_ref, feats_ref, w_ref, dealt_ref,
    natural, mine, theirs, w_mine, w_theirs, x_out, x_in, x_scale_out, x_scale_in, packed, done,
    load_sem, w_load_sem, w_send, w_recv, f_send, f_recv, x_send, x_recv, s_send, s_recv,
    o_send, o_recv, own_sem,
):
    me = lax.axis_index("gx")
    place = lax.axis_index("gy")
    across = place // 2
    core = place % 2
    other_across, other_core = 1 - across, 1 - core
    core_mate = (me, across * 2 + other_core)
    x_mate = (me, other_across * 2 + core)
    share = w_mine.shape[2]
    total = w_ref.shape[1] // 2
    steps = groups * slots

    def columns(block, of_core):
        chip = other_across if block < 2 else across
        first = (block % 2) * total + (chip * 2 + of_core) * share
        return pl.ds(pl.multiple_of(first, 128), share)

    load = pltpu.make_async_copy(feats_ref, natural, load_sem)
    load.start()
    w_loads = [
        pltpu.make_async_copy(w_ref.at[:, columns(b, core)], w_mine.at[b], w_load_sem.at[b])
        for b in range(4)
    ]
    for copy in w_loads:
        copy.start()

    barrier = pltpu.get_barrier_semaphore()
    for mate in (core_mate, x_mate):
        pl.semaphore_signal(barrier, inc=1, device_id=mate, device_id_type=MESH)
    for ahead in range(1, groups):
        pl.semaphore_signal(
            barrier, inc=1, device_id=((me + ahead) % groups, place), device_id_type=MESH
        )
    pl.semaphore_wait(barrier, groups + 1)

    w_copies = [
        pltpu.make_async_remote_copy(
            src_ref=w_ref.at[:, columns(b, other_core)],
            dst_ref=w_theirs.at[b],
            send_sem=w_send.at[b],
            recv_sem=w_recv.at[b],
            device_id=core_mate,
            device_id_type=MESH,
        )
        for b in range(4)
    ]

    def f_copy(k):
        return pltpu.make_async_remote_copy(
            src_ref=mine.at[k], dst_ref=theirs.at[k], send_sem=f_send.at[k],
            recv_sem=f_recv.at[k], device_id=core_mate, device_id_type=MESH,
        )

    def x_copy(k):
        return pltpu.make_async_remote_copy(
            src_ref=x_out.at[k], dst_ref=x_in.at[k], send_sem=x_send.at[k],
            recv_sem=x_recv.at[k], device_id=x_mate, device_id_type=MESH,
        )

    def s_copy(k):
        return pltpu.make_async_remote_copy(
            src_ref=x_scale_out.at[k], dst_ref=x_scale_in.at[k], send_sem=s_send.at[k],
            recv_sem=s_recv.at[k], device_id=x_mate, device_id_type=MESH,
        )

    def o_copy(k, target, landing):
        return pltpu.make_async_remote_copy(
            src_ref=done.at[k], dst_ref=dealt_ref.at[landing], send_sem=o_send.at[k],
            recv_sem=o_recv.at[landing], device_id=(target, place), device_id_type=MESH,
        )

    w_copies[0].start()
    w_copies[1].start()
    load.wait()

    def order(j, carry):
        for part in range(TILE // PIECE):
            mine[j, part * PIECE : (part + 1) * PIECE, :] = natural[
                source_ref[j * (TILE // PIECE) + part]
            ]
        f_copy(j).start()
        return carry

    lax.fori_loop(0, chunks, order, 0)
    w_copies[2].start()
    w_copies[3].start()

    def partial(k, block):
        return jnp.dot(
            mine[k], w_mine[block], preferred_element_type=jnp.float32
        ) + jnp.dot(theirs[k], w_theirs[block], preferred_element_type=jnp.float32)

    for b in range(2):
        w_loads[b].wait()
        w_copies[b].wait_recv()

    heads = 2 * share // HD

    def outward(k):
        f_copy(k).wait_recv()
        lane = lax.broadcasted_iota(jnp.int32, (TILE, HD), 1)
        peaks = jnp.zeros((TILE, HD), jnp.float32)
        for block in range(2):
            sums = partial(k, block)
            for h in range(heads // 2):
                one = sums[:, h * HD : (h + 1) * HD]
                peak = jnp.maximum(jnp.max(jnp.abs(one), axis=-1, keepdims=True), LEAST)
                place = block * (heads // 2) + h
                coded = jnp.round(one * (STEPS / peak)).astype(jnp.int32)
                x_out[k, :, place * HD : (place + 1) * HD] = coded.astype(jnp.int16)
                peaks = jnp.where(lane == place, peak, peaks)
        x_scale_out[k] = jnp.transpose(peaks)[:SCALES]
        s_copy(k).start()
        x_copy(k).start()

    def arrived(j):
        s_copy(j).wait_recv()
        peaks = jnp.transpose(jnp.concatenate([x_scale_in[j]] * (HD // SCALES), axis=0))
        x_copy(j).wait_recv()
        return [
            x_in[j, :, h * HD : (h + 1) * HD].astype(jnp.float32)
            * (peaks[:, h : h + 1] * (1.0 / STEPS))
            for h in range(heads)
        ]

    def finish(j):
        key_part = partial(j, 2)
        value_part = partial(j, 3)
        other = arrived(j)
        parts = TILE // PIECE
        rows = pl.ds(j * parts, parts)
        for h in range(share // HD):
            head = slice(h * HD, (h + 1) * HD)
            one = key_part[:, head] + other[h]
            mean_square = jnp.mean(one * one, axis=-1, keepdims=True)
            normed = one * lax.rsqrt(mean_square + epsilon) * gain_ref[...]
            packed[rows, :, head] = normed.astype(jnp.bfloat16).reshape(parts, PIECE, HD)
            value_pre = value_part[:, head] + other[share // HD + h]
            packed[rows, :, share + h * HD : share + (h + 1) * HD] = value_pre.astype(
                jnp.bfloat16
            ).reshape(parts, PIECE, HD)

    def assemble(k):
        position = lax.broadcasted_iota(jnp.int32, (PIECE, 2 * share), 0)
        limit = limit_ref[k]
        for part in range(TILE // PIECE):
            held = packed[piece_ref[k * (TILE // PIECE) + part]]
            kept = jnp.where(position < limit - part * PIECE, held.astype(jnp.float32), 0.0)
            done[k, part * PIECE : (part + 1) * PIECE, :] = kept.astype(jnp.bfloat16)

    def dispatch(k, carry):
        assemble(k)
        target, cls = route(k, me, groups, slots)
        o_copy(k, target, me * slots + cls).start()
        return carry

    def start(k, carry):
        outward(k)
        return carry

    def inward(k, carry):
        finish(k)
        return dispatch(k, carry)

    def both(k, carry):
        outward(k)
        return inward(k - LEAD, carry)

    leaving = steps - slots
    together = min(chunks, leaving)
    lax.fori_loop(0, LEAD, start, 0)
    for b in range(2, 4):
        w_loads[b].wait()
        w_copies[b].wait_recv()
    lax.fori_loop(LEAD, chunks, both, 0)
    lax.fori_loop(chunks - LEAD, together, inward, 0)
    for j in range(together, chunks):
        finish(j)
    if together < leaving:
        lax.fori_loop(together, leaving, dispatch, 0)
    own = []
    for c in range(slots):
        k = leaving + c
        assemble(k)
        own.append(
            pltpu.make_async_copy(done.at[k], dealt_ref.at[me * slots + c], own_sem.at[c])
        )
        own[-1].start()

    for copy in w_copies:
        copy.wait_send()

    def drain(k, carry):
        f_copy(k).wait_send()
        x_copy(k).wait_send()
        s_copy(k).wait_send()
        return carry

    lax.fori_loop(0, chunks, drain, 0)

    def drain_out(k, carry):
        target, cls = route(k, me, groups, slots)
        o_copy(k, target, me * slots + cls).wait_send()
        o_copy(k, target, target * slots + cls).wait_recv()
        return carry

    lax.fori_loop(0, steps - slots, drain_out, 0)
    for copy in own:
        copy.wait()


def place_kernel(groups, slots, deal_ref, dealt_ref, keys_ref, values_ref, out_sem):
    me = lax.axis_index("gx")
    share = keys_ref.shape[1]
    stores = []
    for s in range(TPD):
        landing = deal_ref[me, s] // TPD * slots + s // groups
        for which, out in enumerate((keys_ref, values_ref)):
            stores.append(
                pltpu.make_async_copy(
                    dealt_ref.at[landing, :, pl.ds(which * share, share)],
                    out.at[pl.ds(s * TILE, TILE), :],
                    out_sem.at[which, s],
                )
            )
            stores[-1].start()
    for copy in stores:
        copy.wait()


def kernel_local(image_feats, w_kv, k_gain, tile_rows, deal):
    groups = lax.axis_size("gx")
    slots = TPD // groups
    width = image_feats.shape[1]
    share = w_kv.shape[1] // 2 // lax.axis_size("gy")
    steps = TPD
    bf16, f32 = jnp.bfloat16, jnp.float32
    smem = pl.BlockSpec(memory_space=pltpu.SMEM)
    anywhere = pl.BlockSpec(memory_space=pl.ANY)
    dma = pltpu.SemaphoreType.DMA

    def project(chunks, call):
        return pl.pallas_call(
            functools.partial(project_kernel, groups, slots, chunks),
            out_shape=jax.ShapeDtypeStruct((TPD, TILE, 2 * share), bf16),
            in_specs=[smem, smem, smem, pl.BlockSpec(memory_space=pltpu.VMEM), anywhere, anywhere],
            out_specs=anywhere,
            scratch_shapes=[
                pltpu.VMEM((TPD * TILE // PIECE, PIECE, width), bf16),
                pltpu.VMEM((chunks, TILE, width), bf16),
                pltpu.VMEM((chunks, TILE, width), bf16),
                pltpu.VMEM((4, width, share), bf16),
                pltpu.VMEM((4, width, share), bf16),
                pltpu.VMEM((chunks, TILE, 2 * share), jnp.int16),
                pltpu.VMEM((chunks, TILE, 2 * share), jnp.int16),
                pltpu.VMEM((chunks, SCALES, HD), f32),
                pltpu.VMEM((chunks, SCALES, HD), f32),
                pltpu.VMEM((chunks * TILE // PIECE, PIECE, 2 * share), bf16),
                pltpu.VMEM((steps, TILE, 2 * share), bf16),
                dma, dma((4,)), dma((4,)), dma((4,)), dma((chunks,)), dma((chunks,)),
                dma((chunks,)), dma((chunks,)), dma((chunks,)), dma((chunks,)),
                dma((steps,)), dma((steps,)), dma((slots,)),
            ],
            compiler_params=pltpu.CompilerParams(collective_id=call, has_side_effects=True),
            name=f"project_and_deal_{chunks}",
        )

    sizes = (TPD * 11 // 16, TPD * 3 // 4, TPD)
    pieces = jnp.maximum((tile_rows + PIECE - 1) // PIECE, 1).reshape(groups, TPD)
    fullest = jnp.max(jnp.sum(pieces, axis=1))
    branch = sum((fullest > size * (TILE // PIECE)).astype(jnp.int32) for size in sizes[:-1])
    dealt = lax.switch(
        branch,
        [project(size, call) for call, size in enumerate(sizes)],
        *tables(lax.axis_index("gx"), groups, slots, tile_rows, deal),
        k_gain.reshape(1, HD), image_feats.reshape(-1, PIECE, width), w_kv,
    )
    result = jax.ShapeDtypeStruct((TPD * TILE, share), bf16)
    return pl.pallas_call(
        functools.partial(place_kernel, groups, slots),
        out_shape=(result, result),
        in_specs=[smem, pl.BlockSpec(memory_space=pltpu.VMEM)],
        out_specs=(anywhere, anywhere),
        scratch_shapes=[dma((2, TPD))],
        name="place_tiles",
    )(deal, dealt)


def solution(mesh):
    groups, width_parts = mesh.shape["gx"], mesh.shape["gy"]
    direct = groups > 1 and TPD % groups == 0 and width_parts == 4
    local = kernel_local if direct else plain_local
    placed = (P("gx", "gy"), P("gy", None), P(), P(), P())
    return jax.shard_map(
        local, mesh=mesh, in_specs=placed, out_specs=(P("gx", "gy"), P("gx", "gy")), check_vma=False
    )
```

```python
import functools

import jax
import jax.numpy as jnp
from jax import lax
from jax.experimental import pallas as pl
from jax.experimental.pallas import tpu as pltpu
from jax.sharding import PartitionSpec as P

HD = 128
TILE = 128
TPD = 16


epsilon = 1e-05


def plain_local(image_feats, w_kv, k_gain, tile_rows, deal):
    local_width = image_feats.shape[1]
    groups = lax.axis_size("gx")
    own_index = lax.axis_index("gx")
    slots = max(1, TPD // groups)
    wanted = lax.dynamic_index_in_dim(deal, own_index, 0, keepdims=False)
    slot_index = jnp.arange(TPD, dtype=jnp.int32)
    slot_class = slot_index // groups
    places = jnp.arange(slots, dtype=jnp.int32)
    class_match = slot_class[None, :] == places[:, None]
    own_tiles = own_index * TPD + slot_index
    sending = deal == own_tiles[None, :]
    send_select = (sending[:, None, :] & class_match[None, :, :]).astype(jnp.bfloat16)
    blocks = image_feats.reshape(TPD, TILE, local_width)
    outgoing = jnp.einsum(
        "dcs,str->dctr", send_select, blocks, preferred_element_type=jnp.float32
    ).astype(jnp.bfloat16)
    incoming = lax.all_to_all(outgoing, "gx", split_axis=0, concat_axis=0, tiled=True)
    sources = jnp.arange(groups, dtype=jnp.int32)
    from_source = (wanted // TPD)[:, None] == sources[None, :]
    take_select = (from_source[:, :, None] & class_match.T[:, None, :]).astype(jnp.bfloat16)
    dealt_tiles = jnp.einsum(
        "snc,nctr->str", take_select, incoming, preferred_element_type=jnp.float32
    ).astype(jnp.bfloat16)
    row_count = TPD * TILE
    dealt_rows = dealt_tiles.reshape(row_count, local_width)
    total_kv = w_kv.shape[1] // 2
    partial_value = jnp.dot(dealt_rows, w_kv, preferred_element_type=jnp.float32)
    projected = lax.psum_scatter(
        partial_value.reshape(row_count, 2, total_kv), "gy", scatter_dimension=2, tiled=True
    )
    share_cols = projected.shape[2]
    key_pre = projected[:, 0, :].reshape(row_count, share_cols // HD, HD)
    value_pre = projected[:, 1, :]
    mean_square = jnp.mean(key_pre * key_pre, axis=-1, keepdims=True)
    normed = (key_pre * lax.rsqrt(mean_square + epsilon) * k_gain).reshape(row_count, share_cols)
    all_tiles = jnp.arange(tile_rows.shape[0], dtype=jnp.int32)
    limits = jnp.sum(
        jnp.where(wanted[:, None] == all_tiles[None, :], tile_rows[None, :], 0), axis=1
    )
    position = jnp.arange(TILE, dtype=jnp.int32)
    valid_rows = (position[None, :] < limits[:, None]).reshape(row_count, 1)
    keys_out = jnp.where(valid_rows, normed, 0.0).astype(jnp.bfloat16)
    values_out = jnp.where(valid_rows, value_pre, 0.0).astype(jnp.bfloat16)
    return (keys_out, values_out)


MESH = pl.DeviceIdType.MESH
SCALES = 8
STEPS = 32767.0
LEAST = 1e-30
AHEAD = 4
LEAD = 3


def route(step, me, groups, slots):
    flips = groups - 1 - step // slots
    target, bit = 0, 1
    while bit < groups:
        target += (me // bit + flips // bit) % 2 * bit
        bit *= 2
    return target, step % slots


def project_kernel(
    groups, slots, rows_ref, deal_ref, gain_ref, feats_ref, w_ref, dealt_ref,
    natural, mine, theirs, w_mine, w_theirs, x_out, x_in, x_scale_out, x_scale_in, done,
    load_sem, w_load_sem, w_send, w_recv, f_send, f_recv, x_send, x_recv, s_send, s_recv,
    o_send, o_recv, own_sem,
):
    me = lax.axis_index("gx")
    place = lax.axis_index("gy")
    across = place // 2
    core = place % 2
    other_across, other_core = 1 - across, 1 - core
    core_mate = (me, across * 2 + other_core)
    x_mate = (me, other_across * 2 + core)
    share = w_mine.shape[2]
    total = w_ref.shape[1] // 2
    heads = 2 * share // HD
    steps = groups * slots
    leaving = steps - slots

    def columns(block, of_core):
        chip = other_across if block < 2 else across
        first = (block % 2) * total + (chip * 2 + of_core) * share
        return pl.ds(pl.multiple_of(first, 128), share)

    load = pltpu.make_async_copy(feats_ref, natural, load_sem)
    load.start()
    w_loads = [
        pltpu.make_async_copy(w_ref.at[:, columns(b, core)], w_mine.at[b], w_load_sem.at[b])
        for b in range(4)
    ]
    for copy in w_loads:
        copy.start()

    barrier = pltpu.get_barrier_semaphore()
    for mate in (core_mate, x_mate):
        pl.semaphore_signal(barrier, inc=1, device_id=mate, device_id_type=MESH)
    for ahead in range(1, groups):
        pl.semaphore_signal(
            barrier, inc=1, device_id=((me + ahead) % groups, place), device_id_type=MESH
        )
    pl.semaphore_wait(barrier, groups + 1)

    w_copies = [
        pltpu.make_async_remote_copy(
            src_ref=w_ref.at[:, columns(b, other_core)],
            dst_ref=w_theirs.at[b],
            send_sem=w_send.at[b],
            recv_sem=w_recv.at[b],
            device_id=core_mate,
            device_id_type=MESH,
        )
        for b in range(4)
    ]

    def f_copy(k):
        return pltpu.make_async_remote_copy(
            src_ref=mine.at[k], dst_ref=theirs.at[k], send_sem=f_send.at[k],
            recv_sem=f_recv.at[k], device_id=core_mate, device_id_type=MESH,
        )

    def x_copy(k):
        return pltpu.make_async_remote_copy(
            src_ref=x_out.at[k], dst_ref=x_in.at[k], send_sem=x_send.at[k],
            recv_sem=x_recv.at[k], device_id=x_mate, device_id_type=MESH,
        )

    def s_copy(k):
        return pltpu.make_async_remote_copy(
            src_ref=x_scale_out.at[k], dst_ref=x_scale_in.at[k], send_sem=s_send.at[k],
            recv_sem=s_recv.at[k], device_id=x_mate, device_id_type=MESH,
        )

    def o_copy(k, target, landing):
        return pltpu.make_async_remote_copy(
            src_ref=done.at[k], dst_ref=dealt_ref.at[landing], send_sem=o_send.at[k],
            recv_sem=o_recv.at[landing], device_id=(target, place), device_id_type=MESH,
        )

    def own_tile(k):
        target, cls = route(k, me, groups, slots)
        slot = 0
        for column in range(groups):
            tile = deal_ref[target, cls * groups + column]
            slot = jnp.where(tile // TPD == me, tile % TPD, slot)
        return slot

    def order(k):
        mine[k] = natural[own_tile(k)]
        f_copy(k).start()

    w_copies[0].start()
    w_copies[1].start()
    load.wait()
    for k in range(AHEAD):
        order(k)
        if k == 1:
            w_copies[2].start()
            w_copies[3].start()

    def partial(k, block):
        return jnp.dot(
            mine[k], w_mine[block], preferred_element_type=jnp.float32
        ) + jnp.dot(theirs[k], w_theirs[block], preferred_element_type=jnp.float32)

    for b in range(2):
        w_loads[b].wait()
        w_copies[b].wait_recv()

    def outward(k):
        f_copy(k).wait_recv()
        lane = lax.broadcasted_iota(jnp.int32, (TILE, HD), 1)
        peaks = jnp.zeros((TILE, HD), jnp.float32)
        for block in range(2):
            sums = partial(k, block)
            for h in range(heads // 2):
                one = sums[:, h * HD : (h + 1) * HD]
                peak = jnp.maximum(jnp.max(jnp.abs(one), axis=-1, keepdims=True), LEAST)
                at = block * (heads // 2) + h
                coded = jnp.round(one * (STEPS / peak)).astype(jnp.int32)
                x_out[k, :, at * HD : (at + 1) * HD] = coded.astype(jnp.int16)
                peaks = jnp.where(lane == at, peak, peaks)
        x_scale_out[k] = jnp.transpose(peaks)[:SCALES]
        s_copy(k).start()
        x_copy(k).start()

    def finish(k):
        key_part = partial(k, 2)
        value_part = partial(k, 3)
        s_copy(k).wait_recv()
        peaks = jnp.transpose(jnp.concatenate([x_scale_in[k]] * (HD // SCALES), axis=0))
        x_copy(k).wait_recv()
        limit = rows_ref[me * TPD + own_tile(k)]
        kept = lax.broadcasted_iota(jnp.int32, (TILE, HD), 0) < limit
        for at in range(heads):
            other = x_in[k, :, at * HD : (at + 1) * HD].astype(jnp.float32)
            other = other * (peaks[:, at : at + 1] * (1.0 / STEPS))
            head = at % (heads // 2)
            part = key_part if at < heads // 2 else value_part
            one = part[:, head * HD : (head + 1) * HD] + other
            if at < heads // 2:
                mean_square = jnp.mean(one * one, axis=-1, keepdims=True)
                one = one * lax.rsqrt(mean_square + epsilon) * gain_ref[...]
            done[k, :, at * HD : (at + 1) * HD] = jnp.where(kept, one, 0.0).astype(jnp.bfloat16)

    def inward(k):
        finish(k)
        target, cls = route(k, me, groups, slots)
        o_copy(k, target, me * slots + cls).start()

    def opening(k, carry):
        order(k + AHEAD)
        outward(k)
        return carry

    def middle(k, carry):
        @pl.when(k + AHEAD < steps)
        def _():
            order(k + AHEAD)

        outward(k)
        inward(k - LEAD)
        return carry

    def closing(k, carry):
        inward(k)
        return carry

    lax.fori_loop(0, LEAD, opening, 0)
    for b in range(2, 4):
        w_loads[b].wait()
        w_copies[b].wait_recv()
    lax.fori_loop(LEAD, steps, middle, 0)
    lax.fori_loop(steps - LEAD, leaving, closing, 0)
    own = []
    for c in range(slots):
        finish(leaving + c)
        own.append(
            pltpu.make_async_copy(
                done.at[leaving + c], dealt_ref.at[me * slots + c], own_sem.at[c]
            )
        )
        own[-1].start()

    for copy in w_copies:
        copy.wait_send()

    def drain(k, carry):
        f_copy(k).wait_send()
        x_copy(k).wait_send()
        s_copy(k).wait_send()
        return carry

    lax.fori_loop(0, steps, drain, 0)

    def drain_out(k, carry):
        target, cls = route(k, me, groups, slots)
        o_copy(k, target, me * slots + cls).wait_send()
        o_copy(k, target, target * slots + cls).wait_recv()
        return carry

    lax.fori_loop(0, leaving, drain_out, 0)
    for copy in own:
        copy.wait()


def place_kernel(groups, slots, deal_ref, dealt_ref, keys_ref, values_ref, out_sem):
    me = lax.axis_index("gx")
    share = keys_ref.shape[1]
    stores = []
    for s in range(TPD):
        landing = deal_ref[me, s] // TPD * slots + s // groups
        for which, out in enumerate((keys_ref, values_ref)):
            stores.append(
                pltpu.make_async_copy(
                    dealt_ref.at[landing, :, pl.ds(which * share, share)],
                    out.at[pl.ds(s * TILE, TILE), :],
                    out_sem.at[which, s],
                )
            )
            stores[-1].start()
    for copy in stores:
        copy.wait()


def kernel_local(image_feats, w_kv, k_gain, tile_rows, deal):
    groups = lax.axis_size("gx")
    slots = TPD // groups
    width = image_feats.shape[1]
    share = w_kv.shape[1] // 2 // lax.axis_size("gy")
    steps = TPD
    bf16, f32 = jnp.bfloat16, jnp.float32
    smem = pl.BlockSpec(memory_space=pltpu.SMEM)
    anywhere = pl.BlockSpec(memory_space=pl.ANY)
    dma = pltpu.SemaphoreType.DMA

    dealt = pl.pallas_call(
        functools.partial(project_kernel, groups, slots),
        out_shape=jax.ShapeDtypeStruct((steps, TILE, 2 * share), bf16),
        in_specs=[smem, smem, pl.BlockSpec(memory_space=pltpu.VMEM), anywhere, anywhere],
        out_specs=anywhere,
        scratch_shapes=[
            pltpu.VMEM((steps, TILE, width), bf16),
            pltpu.VMEM((steps, TILE, width), bf16),
            pltpu.VMEM((steps, TILE, width), bf16),
            pltpu.VMEM((4, width, share), bf16),
            pltpu.VMEM((4, width, share), bf16),
            pltpu.VMEM((steps, TILE, 2 * share), jnp.int16),
            pltpu.VMEM((steps, TILE, 2 * share), jnp.int16),
            pltpu.VMEM((steps, SCALES, HD), f32),
            pltpu.VMEM((steps, SCALES, HD), f32),
            pltpu.VMEM((steps, TILE, 2 * share), bf16),
            dma, dma((4,)), dma((4,)), dma((4,)),
            *[dma((steps,)) for _ in range(8)], dma((slots,)),
        ],
        compiler_params=pltpu.CompilerParams(collective_id=0, has_side_effects=True),
        name="project_and_deal",
    )(tile_rows, deal, k_gain.reshape(1, HD), image_feats.reshape(steps, TILE, width), w_kv)
    result = jax.ShapeDtypeStruct((TPD * TILE, share), bf16)
    return pl.pallas_call(
        functools.partial(place_kernel, groups, slots),
        out_shape=(result, result),
        in_specs=[smem, pl.BlockSpec(memory_space=pltpu.VMEM)],
        out_specs=(anywhere, anywhere),
        scratch_shapes=[dma((2, TPD))],
        name="place_tiles",
    )(deal, dealt)


def solution(mesh):
    groups, width_parts = mesh.shape["gx"], mesh.shape["gy"]
    direct = groups > 1 and TPD % groups == 0 and width_parts == 4
    local = kernel_local if direct else plain_local
    placed = (P("gx", "gy"), P("gy", None), P(), P(), P())
    return jax.shard_map(
        local, mesh=mesh, in_specs=placed, out_specs=(P("gx", "gy"), P("gx", "gy")), check_vma=False
    )
```

```python
import functools

import jax
import jax.numpy as jnp
from jax import lax
from jax.experimental import pallas as pl
from jax.experimental.pallas import tpu as pltpu
from jax.sharding import PartitionSpec as P

HD = 128
TILE = 128
TPD = 16


epsilon = 1e-05


def plain_local(image_feats, w_kv, k_gain, tile_rows, deal):
    local_width = image_feats.shape[1]
    groups = lax.axis_size("gx")
    own_index = lax.axis_index("gx")
    slots = max(1, TPD // groups)
    wanted = lax.dynamic_index_in_dim(deal, own_index, 0, keepdims=False)
    slot_index = jnp.arange(TPD, dtype=jnp.int32)
    slot_class = slot_index // groups
    places = jnp.arange(slots, dtype=jnp.int32)
    class_match = slot_class[None, :] == places[:, None]
    own_tiles = own_index * TPD + slot_index
    sending = deal == own_tiles[None, :]
    send_select = (sending[:, None, :] & class_match[None, :, :]).astype(jnp.bfloat16)
    blocks = image_feats.reshape(TPD, TILE, local_width)
    outgoing = jnp.einsum(
        "dcs,str->dctr", send_select, blocks, preferred_element_type=jnp.float32
    ).astype(jnp.bfloat16)
    incoming = lax.all_to_all(outgoing, "gx", split_axis=0, concat_axis=0, tiled=True)
    sources = jnp.arange(groups, dtype=jnp.int32)
    from_source = (wanted // TPD)[:, None] == sources[None, :]
    take_select = (from_source[:, :, None] & class_match.T[:, None, :]).astype(jnp.bfloat16)
    dealt_tiles = jnp.einsum(
        "snc,nctr->str", take_select, incoming, preferred_element_type=jnp.float32
    ).astype(jnp.bfloat16)
    row_count = TPD * TILE
    dealt_rows = dealt_tiles.reshape(row_count, local_width)
    total_kv = w_kv.shape[1] // 2
    partial_value = jnp.dot(dealt_rows, w_kv, preferred_element_type=jnp.float32)
    projected = lax.psum_scatter(
        partial_value.reshape(row_count, 2, total_kv), "gy", scatter_dimension=2, tiled=True
    )
    share_cols = projected.shape[2]
    key_pre = projected[:, 0, :].reshape(row_count, share_cols // HD, HD)
    value_pre = projected[:, 1, :]
    mean_square = jnp.mean(key_pre * key_pre, axis=-1, keepdims=True)
    normed = (key_pre * lax.rsqrt(mean_square + epsilon) * k_gain).reshape(row_count, share_cols)
    all_tiles = jnp.arange(tile_rows.shape[0], dtype=jnp.int32)
    limits = jnp.sum(
        jnp.where(wanted[:, None] == all_tiles[None, :], tile_rows[None, :], 0), axis=1
    )
    position = jnp.arange(TILE, dtype=jnp.int32)
    valid_rows = (position[None, :] < limits[:, None]).reshape(row_count, 1)
    keys_out = jnp.where(valid_rows, normed, 0.0).astype(jnp.bfloat16)
    values_out = jnp.where(valid_rows, value_pre, 0.0).astype(jnp.bfloat16)
    return (keys_out, values_out)


MESH = pl.DeviceIdType.MESH
SCALES = 8
STEPS = 32767.0
LEAST = 1e-30
AHEAD = 4
LEAD = 2
PARTS = 4


def route(step, me, groups, slots):
    flips = groups - 1 - step // slots
    target, bit = 0, 1
    while bit < groups:
        target += (me // bit + flips // bit) % 2 * bit
        bit *= 2
    return target, step % slots


def project_kernel(
    groups, slots, rows_ref, deal_ref, gain_ref, feats_ref, w_ref, keys_ref, values_ref,
    natural, mine, theirs, w_mine, w_give, w_theirs, x_out, x_in, x_scale_out, x_scale_in,
    done, landed, load_sem, w_load_sem, w_give_sem, w_send, w_recv, f_send, f_recv,
    x_send, x_recv, s_send, s_recv, o_send, o_recv, answer_sem, open_sem,
):
    me = lax.axis_index("gx")
    place = lax.axis_index("gy")
    across = place // 2
    core = place % 2
    other_across, other_core = 1 - across, 1 - core
    core_mate = (me, across * 2 + other_core)
    x_mate = (me, other_across * 2 + core)
    share = w_mine.shape[2]
    total = w_ref.shape[1] // 2
    heads = share // HD
    steps = groups * slots
    leaving = steps - slots

    def columns(block, of_core):
        chip = other_across if block < 2 else across
        first = (block % 2) * total + (chip * 2 + of_core) * share
        return pl.ds(pl.multiple_of(first, 128), share)

    def w_load(b, of_core, into, sem):
        return pltpu.make_async_copy(w_ref.at[:, columns(b, of_core)], into.at[b], sem.at[b])

    load = pltpu.make_async_copy(feats_ref, natural, load_sem)
    w_loads = [w_load(b, core, w_mine, w_load_sem) for b in range(4)]
    w_gives = [w_load(b, other_core, w_give, w_give_sem) for b in range(4)]
    for copy in (*w_gives[:2], load, *w_loads[:2], *w_gives[2:], *w_loads[2:]):
        copy.start()

    barrier = pltpu.get_barrier_semaphore()
    leads = place == 0
    leader = (me, 0)
    knows_leader = (place == 1) | (place == 2)

    @pl.when(~knows_leader)
    def _():
        for mate in (core_mate, x_mate):
            pl.semaphore_signal(barrier, inc=1, device_id=mate, device_id_type=MESH)

    @pl.when(knows_leader)
    def _():
        pl.semaphore_signal(barrier, inc=1, device_id=(me, 3), device_id_type=MESH)

    @pl.when(~leads)
    def _():
        pl.semaphore_wait(barrier, 2)

    @pl.when(knows_leader)
    def _():
        pl.semaphore_signal(answer_sem, inc=1, device_id=leader, device_id_type=MESH)

    @pl.when(leads)
    def _():
        pl.semaphore_wait(answer_sem, 2)
        for ahead in range(1, groups):
            pl.semaphore_signal(
                barrier, inc=1, device_id=((me + ahead) % groups, 0), device_id_type=MESH
            )

    def open_deal():
        pl.semaphore_wait(barrier, groups - 1)
        for mate in range(1, 4):
            pl.semaphore_signal(open_sem, inc=1, device_id=(me, mate), device_id_type=MESH)

    w_copies = [
        pltpu.make_async_remote_copy(
            src_ref=w_give.at[b],
            dst_ref=w_theirs.at[b],
            send_sem=w_send.at[b],
            recv_sem=w_recv.at[b],
            device_id=core_mate,
            device_id_type=MESH,
        )
        for b in range(4)
    ]

    def send_weights(b):
        w_gives[b].wait()
        w_copies[b].start()

    def f_copy(k):
        return pltpu.make_async_remote_copy(
            src_ref=mine.at[k], dst_ref=theirs.at[k], send_sem=f_send.at[k],
            recv_sem=f_recv.at[k], device_id=core_mate, device_id_type=MESH,
        )

    def x_copy(b, k):
        return pltpu.make_async_remote_copy(
            src_ref=x_out.at[b, k], dst_ref=x_in.at[b, k], send_sem=x_send.at[b, k],
            recv_sem=x_recv.at[b, k], device_id=x_mate, device_id_type=MESH,
        )

    def s_copy(b, k):
        return pltpu.make_async_remote_copy(
            src_ref=x_scale_out.at[b, k], dst_ref=x_scale_in.at[b, k], send_sem=s_send.at[b, k],
            recv_sem=s_recv.at[b, k], device_id=x_mate, device_id_type=MESH,
        )

    def o_copy(b, k, target, landing):
        return pltpu.make_async_remote_copy(
            src_ref=done.at[b, k], dst_ref=landed.at[b, landing], send_sem=o_send.at[b, k],
            recv_sem=o_recv.at[b, landing], device_id=(target, place), device_id_type=MESH,
        )

    def own_tile(k):
        target, cls = route(k, me, groups, slots)
        slot = 0
        for column in range(groups):
            tile = deal_ref[target, cls * groups + column]
            slot = jnp.where(tile // TPD == me, tile % TPD, slot)
        return slot

    def order(k):
        mine[k] = natural[own_tile(k)]
        f_copy(k).start()

    send_weights(0)
    load.wait()
    order(0)
    send_weights(1)
    order(1)
    send_weights(2)
    send_weights(3)
    for k in range(2, AHEAD):
        order(k)

    def partial(k, block):
        return jnp.dot(
            mine[k], w_mine[block], preferred_element_type=jnp.float32
        ) + jnp.dot(theirs[k], w_theirs[block], preferred_element_type=jnp.float32)

    def weights_here(b):
        w_loads[b].wait()
        w_copies[b].wait_recv()

    def outward(k, first):
        f_copy(k).wait_recv()
        lane = lax.broadcasted_iota(jnp.int32, (TILE, HD), 1)
        for b in range(2):
            if first:
                weights_here(b)
            sums = partial(k, b)
            peaks = jnp.zeros((TILE, HD), jnp.float32)
            for h in range(heads):
                one = sums[:, h * HD : (h + 1) * HD]
                peak = jnp.maximum(jnp.max(jnp.abs(one), axis=-1, keepdims=True), LEAST)
                coded = jnp.round(one * (STEPS / peak)).astype(jnp.int32)
                x_out[b, k, :, h * HD : (h + 1) * HD] = coded.astype(jnp.int16)
                peaks = jnp.where(lane == h, peak, peaks)
            x_scale_out[b, k] = jnp.transpose(peaks)[:SCALES]
            s_copy(b, k).start()
            x_copy(b, k).start()

    def finish(k, send):
        limit = rows_ref[me * TPD + own_tile(k)]
        kept = lax.broadcasted_iota(jnp.int32, (TILE, HD), 0) < limit
        target, cls = route(k, me, groups, slots)
        for b in range(2):
            part = partial(k, 2 + b)
            s_copy(b, k).wait_recv()
            peaks = jnp.transpose(jnp.concatenate([x_scale_in[b, k]] * (HD // SCALES), axis=0))
            x_copy(b, k).wait_recv()
            for h in range(heads):
                head = slice(h * HD, (h + 1) * HD)
                other = x_in[b, k, :, head].astype(jnp.float32)
                one = part[:, head] + other * (peaks[:, h : h + 1] * (1.0 / STEPS))
                if b == 0:
                    mean_square = jnp.mean(one * one, axis=-1, keepdims=True)
                    one = one * lax.rsqrt(mean_square + epsilon) * gain_ref[...]
                done[b, k, :, head] = jnp.where(kept, one, 0.0).astype(jnp.bfloat16)
            if send:
                o_copy(b, k, target, me * slots + cls).start()
            else:
                landed[b, target * slots + cls] = done[b, k]

    def opening(k, carry):
        order(k + AHEAD)
        outward(k, False)
        return carry

    def middle(k, carry):
        @pl.when(k + AHEAD < steps)
        def _():
            order(k + AHEAD)

        outward(k, False)
        finish(k - LEAD, True)
        return carry

    def closing(k, carry):
        finish(k, True)
        return carry

    outward(0, True)
    pl.when(leads)(open_deal)
    order(AHEAD)
    lax.fori_loop(1, LEAD, opening, 0)
    for b in range(2, 4):
        weights_here(b)

    @pl.when(~leads)
    def _():
        pl.semaphore_wait(open_sem, 1)

    lax.fori_loop(LEAD, steps, middle, 0)
    lax.fori_loop(steps - LEAD, leaving, closing, 0)
    for c in range(slots):
        finish(leaving + c, False)

    for copy in w_copies:
        copy.wait_send()

    def drain(k, carry):
        f_copy(k).wait_send()
        for b in range(2):
            x_copy(b, k).wait_send()
            s_copy(b, k).wait_send()
        return carry

    lax.fori_loop(0, steps, drain, 0)

    def drain_out(k, carry):
        target, cls = route(k, me, groups, slots)
        for b in range(2):
            o_copy(b, k, target, me * slots + cls).wait_send()
            o_copy(b, k, target, target * slots + cls).wait_recv()
        return carry

    lax.fori_loop(0, leaving, drain_out, 0)

    def settle(tile, carry):
        landing = deal_ref[me, tile] // TPD * slots + tile // groups
        rows = pl.ds(pl.multiple_of(tile * TILE, TILE), TILE)
        keys_ref[rows, :] = landed[0, landing]
        values_ref[rows, :] = landed[1, landing]
        return carry

    lax.fori_loop(0, TPD, settle, 0)


def store_kernel(keys_ref, values_ref, keys_out, values_out, sem):
    parts = keys_ref.shape[0] // PARTS
    stores = []
    for which, (source, out) in enumerate(((keys_ref, keys_out), (values_ref, values_out))):
        for part in range(PARTS):
            rows = pl.ds(part * parts, parts)
            stores.append(
                pltpu.make_async_copy(source.at[rows], out.at[rows], sem.at[which, part])
            )
            stores[-1].start()
    for copy in stores:
        copy.wait()


def kernel_local(image_feats, w_kv, k_gain, tile_rows, deal):
    groups = lax.axis_size("gx")
    slots = TPD // groups
    width = image_feats.shape[1]
    share = w_kv.shape[1] // 2 // lax.axis_size("gy")
    steps = TPD
    bf16, f32 = jnp.bfloat16, jnp.float32
    smem = pl.BlockSpec(memory_space=pltpu.SMEM)
    anywhere = pl.BlockSpec(memory_space=pl.ANY)
    dma = pltpu.SemaphoreType.DMA

    tiles = pltpu.VMEM((steps, TILE, width), bf16)
    weights = pltpu.VMEM((4, width, share), bf16)
    codes = pltpu.VMEM((2, steps, TILE, share), jnp.int16)
    scales = pltpu.VMEM((2, steps, SCALES, HD), f32)
    results = pltpu.VMEM((2, steps, TILE, share), bf16)
    result = pltpu.VMEM((TPD * TILE, share), bf16)
    vmem = pl.BlockSpec(memory_space=pltpu.VMEM)
    results = pl.pallas_call(
        functools.partial(project_kernel, groups, slots),
        out_shape=(result, result),
        in_specs=[smem, smem, vmem, anywhere, anywhere],
        out_specs=(vmem, vmem),
        scratch_shapes=[
            tiles, tiles, tiles, weights, weights, weights, codes, codes, scales, scales,
            results, results, dma, dma((4,)), dma((4,)), dma((4,)), dma((4,)),
            dma((steps,)), dma((steps,)), *[dma((2, steps)) for _ in range(6)],
            pltpu.SemaphoreType.REGULAR, pltpu.SemaphoreType.REGULAR,
        ],
        compiler_params=pltpu.CompilerParams(collective_id=0, has_side_effects=True),
        name="project_and_deal",
    )(tile_rows, deal, k_gain.reshape(1, HD), image_feats.reshape(steps, TILE, width), w_kv)
    stored = jax.ShapeDtypeStruct((TPD * TILE, share), bf16)
    return pl.pallas_call(
        store_kernel,
        out_shape=(stored, stored),
        in_specs=[vmem, vmem],
        out_specs=(anywhere, anywhere),
        scratch_shapes=[dma((2, PARTS))],
        name="store_result",
    )(*[pltpu.with_memory_space_constraint(part, pltpu.VMEM) for part in results])


def solution(mesh):
    groups, width_parts = mesh.shape["gx"], mesh.shape["gy"]
    direct = groups > 1 and TPD % groups == 0 and width_parts == 4
    local = kernel_local if direct else plain_local
    placed = (P("gx", "gy"), P("gy", None), P(), P(), P())
    return jax.shard_map(
        local, mesh=mesh, in_specs=placed, out_specs=(P("gx", "gy"), P("gx", "gy")), check_vma=False
    )
```

```python
import functools

import jax
import jax.numpy as jnp
from jax import lax
from jax.experimental import pallas as pl
from jax.experimental.pallas import tpu as pltpu
from jax.sharding import PartitionSpec as P

HD = 128
TILE = 128
TPD = 16


epsilon = 1e-05


def plain_local(image_feats, w_kv, k_gain, tile_rows, deal):
    local_width = image_feats.shape[1]
    groups = lax.axis_size("gx")
    own_index = lax.axis_index("gx")
    slots = max(1, TPD // groups)
    wanted = lax.dynamic_index_in_dim(deal, own_index, 0, keepdims=False)
    slot_index = jnp.arange(TPD, dtype=jnp.int32)
    slot_class = slot_index // groups
    places = jnp.arange(slots, dtype=jnp.int32)
    class_match = slot_class[None, :] == places[:, None]
    own_tiles = own_index * TPD + slot_index
    sending = deal == own_tiles[None, :]
    send_select = (sending[:, None, :] & class_match[None, :, :]).astype(jnp.bfloat16)
    blocks = image_feats.reshape(TPD, TILE, local_width)
    outgoing = jnp.einsum(
        "dcs,str->dctr", send_select, blocks, preferred_element_type=jnp.float32
    ).astype(jnp.bfloat16)
    incoming = lax.all_to_all(outgoing, "gx", split_axis=0, concat_axis=0, tiled=True)
    sources = jnp.arange(groups, dtype=jnp.int32)
    from_source = (wanted // TPD)[:, None] == sources[None, :]
    take_select = (from_source[:, :, None] & class_match.T[:, None, :]).astype(jnp.bfloat16)
    dealt_tiles = jnp.einsum(
        "snc,nctr->str", take_select, incoming, preferred_element_type=jnp.float32
    ).astype(jnp.bfloat16)
    row_count = TPD * TILE
    dealt_rows = dealt_tiles.reshape(row_count, local_width)
    total_kv = w_kv.shape[1] // 2
    partial_value = jnp.dot(dealt_rows, w_kv, preferred_element_type=jnp.float32)
    projected = lax.psum_scatter(
        partial_value.reshape(row_count, 2, total_kv), "gy", scatter_dimension=2, tiled=True
    )
    share_cols = projected.shape[2]
    key_pre = projected[:, 0, :].reshape(row_count, share_cols // HD, HD)
    value_pre = projected[:, 1, :]
    mean_square = jnp.mean(key_pre * key_pre, axis=-1, keepdims=True)
    normed = (key_pre * lax.rsqrt(mean_square + epsilon) * k_gain).reshape(row_count, share_cols)
    all_tiles = jnp.arange(tile_rows.shape[0], dtype=jnp.int32)
    limits = jnp.sum(
        jnp.where(wanted[:, None] == all_tiles[None, :], tile_rows[None, :], 0), axis=1
    )
    position = jnp.arange(TILE, dtype=jnp.int32)
    valid_rows = (position[None, :] < limits[:, None]).reshape(row_count, 1)
    keys_out = jnp.where(valid_rows, normed, 0.0).astype(jnp.bfloat16)
    values_out = jnp.where(valid_rows, value_pre, 0.0).astype(jnp.bfloat16)
    return (keys_out, values_out)


MESH = pl.DeviceIdType.MESH
STEPS = 32767.0
LEAST = 1e-30
AHEAD = 4
LEAD = 2
PARTS = 4


def down(top, bottom):
    return list(range(top - 1, bottom - 1, -1))


def route(step, me, groups, slots):
    turn, quarter = step // slots, groups // 4
    at_end = (me // quarter) % 3 == 0
    outer = down(groups, 0)
    inner = [
        *down(3 * quarter, quarter), *down(groups, 3 * quarter), *down(quarter, 0)
    ]
    flips = 0
    for at, (far, near) in enumerate(zip(outer, inner)):
        flips = jnp.where(turn == at, jnp.where(at_end, far, near), flips)
    target, bit = 0, 1
    while bit < groups:
        target += (me // bit + flips // bit) % 2 * bit
        bit *= 2
    return target, step % slots


def project_kernel(
    groups, slots, rows_ref, deal_ref, gain_ref, feats_ref, w_ref, keys_ref, values_ref,
    natural, mine, theirs, w_mine, w_give, w_theirs, x_out, x_in, x_scale_out, x_scale_in,
    done, landed, load_sem, w_load_sem, w_give_sem, w_send, w_recv, f_send, f_recv,
    x_send, x_recv, s_send, s_recv, o_send, o_recv, answer_sem, open_sem,
):
    me = lax.axis_index("gx")
    place = lax.axis_index("gy")
    across = place // 2
    core = place % 2
    other_across, other_core = 1 - across, 1 - core
    core_mate = (me, across * 2 + other_core)
    x_mate = (me, other_across * 2 + core)
    share = w_mine.shape[2]
    total = w_ref.shape[1] // 2
    heads = share // HD
    steps = groups * slots
    leaving = steps - slots

    def columns(block, of_core):
        chip = other_across if block < 2 else across
        first = (block % 2) * total + (chip * 2 + of_core) * share
        return pl.ds(pl.multiple_of(first, 128), share)

    def w_load(b, of_core, into, sem):
        return pltpu.make_async_copy(w_ref.at[:, columns(b, of_core)], into.at[b], sem.at[b])

    load = pltpu.make_async_copy(feats_ref, natural, load_sem)
    w_loads = [w_load(b, core, w_mine, w_load_sem) for b in range(4)]
    w_gives = [w_load(b, other_core, w_give, w_give_sem) for b in range(4)]
    for copy in (*w_gives[:2], load, *w_loads[:2], *w_gives[2:], *w_loads[2:]):
        copy.start()

    barrier = pltpu.get_barrier_semaphore()
    leads = place == 0
    leader = (me, 0)
    knows_leader = (place == 1) | (place == 2)

    @pl.when(~knows_leader)
    def _():
        for mate in (core_mate, x_mate):
            pl.semaphore_signal(barrier, inc=1, device_id=mate, device_id_type=MESH)

    @pl.when(knows_leader)
    def _():
        pl.semaphore_signal(barrier, inc=1, device_id=(me, 3), device_id_type=MESH)

    @pl.when(~leads)
    def _():
        pl.semaphore_wait(barrier, 2)

    @pl.when(knows_leader)
    def _():
        pl.semaphore_signal(answer_sem, inc=1, device_id=leader, device_id_type=MESH)

    @pl.when(leads)
    def _():
        pl.semaphore_wait(answer_sem, 2)
        for ahead in range(1, groups):
            pl.semaphore_signal(
                barrier, inc=1, device_id=((me + ahead) % groups, 0), device_id_type=MESH
            )

    def open_deal():
        pl.semaphore_wait(barrier, groups - 1)
        for mate in range(1, 4):
            pl.semaphore_signal(open_sem, inc=1, device_id=(me, mate), device_id_type=MESH)

    w_copies = [
        pltpu.make_async_remote_copy(
            src_ref=w_give.at[b],
            dst_ref=w_theirs.at[b],
            send_sem=w_send.at[b],
            recv_sem=w_recv.at[b],
            device_id=core_mate,
            device_id_type=MESH,
        )
        for b in range(4)
    ]

    def send_weights(b):
        w_gives[b].wait()
        w_copies[b].start()

    def f_copy(k):
        return pltpu.make_async_remote_copy(
            src_ref=mine.at[k], dst_ref=theirs.at[k], send_sem=f_send.at[k],
            recv_sem=f_recv.at[k], device_id=core_mate, device_id_type=MESH,
        )

    def x_copy(b, k):
        return pltpu.make_async_remote_copy(
            src_ref=x_out.at[b, k], dst_ref=x_in.at[b, k], send_sem=x_send.at[b, k],
            recv_sem=x_recv.at[b, k], device_id=x_mate, device_id_type=MESH,
        )

    def s_copy(k):
        return pltpu.make_async_remote_copy(
            src_ref=x_scale_out.at[k], dst_ref=x_scale_in.at[k], send_sem=s_send.at[k],
            recv_sem=s_recv.at[k], device_id=x_mate, device_id_type=MESH,
        )

    def o_copy(b, k, target, landing):
        return pltpu.make_async_remote_copy(
            src_ref=done.at[b, k], dst_ref=landed.at[b, landing], send_sem=o_send.at[b, k],
            recv_sem=o_recv.at[b, landing], device_id=(target, place), device_id_type=MESH,
        )

    def own_tile(k):
        target, cls = route(k, me, groups, slots)
        slot = 0
        for column in range(groups):
            tile = deal_ref[target, cls * groups + column]
            slot = jnp.where(tile // TPD == me, tile % TPD, slot)
        return slot

    def order(k):
        mine[k] = natural[own_tile(k)]
        f_copy(k).start()

    send_weights(0)
    load.wait()
    order(0)
    send_weights(1)
    order(1)
    send_weights(2)
    send_weights(3)
    for k in range(2, AHEAD):
        order(k)

    def partial(k, block):
        return jnp.dot(
            mine[k], w_mine[block], preferred_element_type=jnp.float32
        ) + jnp.dot(theirs[k], w_theirs[block], preferred_element_type=jnp.float32)

    def weights_here(b):
        w_loads[b].wait()
        w_copies[b].wait_recv()

    def outward(k, first):
        f_copy(k).wait_recv()
        lane = lax.broadcasted_iota(jnp.int32, (TILE, HD), 1)
        peaks = jnp.zeros((TILE, HD), jnp.float32)
        for b in range(2):
            if first:
                weights_here(b)
            sums = partial(k, b)
            for h in range(heads):
                one = sums[:, h * HD : (h + 1) * HD]
                peak = jnp.maximum(jnp.max(jnp.abs(one), axis=-1, keepdims=True), LEAST)
                coded = jnp.round(one * (STEPS / peak)).astype(jnp.int32)
                x_out[b, k, :, h * HD : (h + 1) * HD] = coded.astype(jnp.int16)
                peaks = jnp.where(lane == b * heads + h, peak, peaks)
            if b == 1:
                x_scale_out[k] = jnp.transpose(peaks)[: 2 * heads]
                s_copy(k).start()
            x_copy(b, k).start()

    def finish(k, send):
        limit = rows_ref[me * TPD + own_tile(k)]
        kept = lax.broadcasted_iota(jnp.int32, (TILE, HD), 0) < limit
        target, cls = route(k, me, groups, slots)
        for b in range(2):
            part = partial(k, 2 + b)
            if b == 0:
                s_copy(k).wait_recv()
                repeats = HD // (2 * heads)
                peaks = jnp.transpose(jnp.concatenate([x_scale_in[k]] * repeats, axis=0))
            x_copy(b, k).wait_recv()
            for h in range(heads):
                head, at = slice(h * HD, (h + 1) * HD), b * heads + h
                other = x_in[b, k, :, head].astype(jnp.float32)
                one = part[:, head] + other * (peaks[:, at : at + 1] * (1.0 / STEPS))
                if b == 0:
                    mean_square = jnp.mean(one * one, axis=-1, keepdims=True)
                    one = one * lax.rsqrt(mean_square + epsilon) * gain_ref[...]
                done[b, k, :, head] = jnp.where(kept, one, 0.0).astype(jnp.bfloat16)
            if send:
                o_copy(b, k, target, me * slots + cls).start()
            else:
                landed[b, target * slots + cls] = done[b, k]

    def opening(k, carry):
        order(k + AHEAD)
        outward(k, False)
        return carry

    def middle(k, carry):
        @pl.when(k + AHEAD < steps)
        def _():
            order(k + AHEAD)

        outward(k, False)
        finish(k - LEAD, True)
        return carry

    def closing(k, carry):
        finish(k, True)
        return carry

    outward(0, True)
    pl.when(leads)(open_deal)
    order(AHEAD)
    lax.fori_loop(1, LEAD, opening, 0)
    for b in range(2, 4):
        weights_here(b)

    @pl.when(~leads)
    def _():
        pl.semaphore_wait(open_sem, 1)

    lax.fori_loop(LEAD, steps, middle, 0)
    lax.fori_loop(steps - LEAD, leaving, closing, 0)
    for c in range(slots):
        finish(leaving + c, False)

    for copy in w_copies:
        copy.wait_send()

    def drain(k, carry):
        f_copy(k).wait_send()
        s_copy(k).wait_send()
        for b in range(2):
            x_copy(b, k).wait_send()
        return carry

    lax.fori_loop(0, steps, drain, 0)

    def drain_out(k, carry):
        target, cls = route(k, me, groups, slots)
        for b in range(2):
            o_copy(b, k, target, me * slots + cls).wait_send()
            o_copy(b, k, target, target * slots + cls).wait_recv()
        return carry

    lax.fori_loop(0, leaving, drain_out, 0)

    def settle(tile, carry):
        landing = deal_ref[me, tile] // TPD * slots + tile // groups
        rows = pl.ds(pl.multiple_of(tile * TILE, TILE), TILE)
        keys_ref[rows, :] = landed[0, landing]
        values_ref[rows, :] = landed[1, landing]
        return carry

    lax.fori_loop(0, TPD, settle, 0)


def store_kernel(keys_ref, values_ref, keys_out, values_out, sem):
    parts = keys_ref.shape[0] // PARTS
    stores = []
    for which, (source, out) in enumerate(((keys_ref, keys_out), (values_ref, values_out))):
        for part in range(PARTS):
            rows = pl.ds(part * parts, parts)
            stores.append(
                pltpu.make_async_copy(source.at[rows], out.at[rows], sem.at[which, part])
            )
            stores[-1].start()
    for copy in stores:
        copy.wait()


def kernel_local(image_feats, w_kv, k_gain, tile_rows, deal):
    groups = lax.axis_size("gx")
    slots = TPD // groups
    width = image_feats.shape[1]
    share = w_kv.shape[1] // 2 // lax.axis_size("gy")
    steps = TPD
    bf16, f32 = jnp.bfloat16, jnp.float32
    smem = pl.BlockSpec(memory_space=pltpu.SMEM)
    anywhere = pl.BlockSpec(memory_space=pl.ANY)
    dma = pltpu.SemaphoreType.DMA

    tiles = pltpu.VMEM((steps, TILE, width), bf16)
    weights = pltpu.VMEM((4, width, share), bf16)
    codes = pltpu.VMEM((2, steps, TILE, share), jnp.int16)
    scales = pltpu.VMEM((steps, 2 * share // HD, HD), f32)
    results = pltpu.VMEM((2, steps, TILE, share), bf16)
    result = pltpu.VMEM((TPD * TILE, share), bf16)
    vmem = pl.BlockSpec(memory_space=pltpu.VMEM)
    results = pl.pallas_call(
        functools.partial(project_kernel, groups, slots),
        out_shape=(result, result),
        in_specs=[smem, smem, vmem, anywhere, anywhere],
        out_specs=(vmem, vmem),
        scratch_shapes=[
            tiles, tiles, tiles, weights, weights, weights, codes, codes, scales, scales,
            results, results, dma, dma((4,)), dma((4,)), dma((4,)), dma((4,)),
            dma((steps,)), dma((steps,)), dma((2, steps)), dma((2, steps)),
            dma((steps,)), dma((steps,)), dma((2, steps)), dma((2, steps)),
            pltpu.SemaphoreType.REGULAR, pltpu.SemaphoreType.REGULAR,
        ],
        compiler_params=pltpu.CompilerParams(collective_id=0, has_side_effects=True),
        name="project_and_deal",
    )(tile_rows, deal, k_gain.reshape(1, HD), image_feats.reshape(steps, TILE, width), w_kv)
    stored = jax.ShapeDtypeStruct((TPD * TILE, share), bf16)
    return pl.pallas_call(
        store_kernel,
        out_shape=(stored, stored),
        in_specs=[vmem, vmem],
        out_specs=(anywhere, anywhere),
        scratch_shapes=[dma((2, PARTS))],
        name="store_result",
    )(*[pltpu.with_memory_space_constraint(part, pltpu.VMEM) for part in results])


def solution(mesh):
    groups, width_parts = mesh.shape["gx"], mesh.shape["gy"]
    direct = groups % 4 == 0 and TPD % groups == 0 and width_parts == 4
    local = kernel_local if direct else plain_local
    placed = (P("gx", "gy"), P("gy", None), P(), P(), P())
    return jax.shard_map(
        local, mesh=mesh, in_specs=placed, out_specs=(P("gx", "gy"), P("gx", "gy")), check_vma=False
    )
```

```python
import functools

import jax
import jax.numpy as jnp
from jax import lax
from jax.experimental import pallas as pl
from jax.experimental.pallas import tpu as pltpu
from jax.sharding import PartitionSpec as P

HD = 128
TILE = 128
TPD = 16


epsilon = 1e-05


def plain_local(image_feats, w_kv, k_gain, tile_rows, deal):
    local_width = image_feats.shape[1]
    groups = lax.axis_size("gx")
    own_index = lax.axis_index("gx")
    slots = max(1, TPD // groups)
    wanted = lax.dynamic_index_in_dim(deal, own_index, 0, keepdims=False)
    slot_index = jnp.arange(TPD, dtype=jnp.int32)
    slot_class = slot_index // groups
    places = jnp.arange(slots, dtype=jnp.int32)
    class_match = slot_class[None, :] == places[:, None]
    own_tiles = own_index * TPD + slot_index
    sending = deal == own_tiles[None, :]
    send_select = (sending[:, None, :] & class_match[None, :, :]).astype(jnp.bfloat16)
    blocks = image_feats.reshape(TPD, TILE, local_width)
    outgoing = jnp.einsum(
        "dcs,str->dctr", send_select, blocks, preferred_element_type=jnp.float32
    ).astype(jnp.bfloat16)
    incoming = lax.all_to_all(outgoing, "gx", split_axis=0, concat_axis=0, tiled=True)
    sources = jnp.arange(groups, dtype=jnp.int32)
    from_source = (wanted // TPD)[:, None] == sources[None, :]
    take_select = (from_source[:, :, None] & class_match.T[:, None, :]).astype(jnp.bfloat16)
    dealt_tiles = jnp.einsum(
        "snc,nctr->str", take_select, incoming, preferred_element_type=jnp.float32
    ).astype(jnp.bfloat16)
    row_count = TPD * TILE
    dealt_rows = dealt_tiles.reshape(row_count, local_width)
    total_kv = w_kv.shape[1] // 2
    partial_value = jnp.dot(dealt_rows, w_kv, preferred_element_type=jnp.float32)
    projected = lax.psum_scatter(
        partial_value.reshape(row_count, 2, total_kv), "gy", scatter_dimension=2, tiled=True
    )
    share_cols = projected.shape[2]
    key_pre = projected[:, 0, :].reshape(row_count, share_cols // HD, HD)
    value_pre = projected[:, 1, :]
    mean_square = jnp.mean(key_pre * key_pre, axis=-1, keepdims=True)
    normed = (key_pre * lax.rsqrt(mean_square + epsilon) * k_gain).reshape(row_count, share_cols)
    all_tiles = jnp.arange(tile_rows.shape[0], dtype=jnp.int32)
    limits = jnp.sum(
        jnp.where(wanted[:, None] == all_tiles[None, :], tile_rows[None, :], 0), axis=1
    )
    position = jnp.arange(TILE, dtype=jnp.int32)
    valid_rows = (position[None, :] < limits[:, None]).reshape(row_count, 1)
    keys_out = jnp.where(valid_rows, normed, 0.0).astype(jnp.bfloat16)
    values_out = jnp.where(valid_rows, value_pre, 0.0).astype(jnp.bfloat16)
    return (keys_out, values_out)


MESH = pl.DeviceIdType.MESH
STEPS = 32767.0
LEAST = 1e-30
AHEAD = 4
LEAD = 2
PARTS = 4


def down(top, bottom):
    return list(range(top - 1, bottom - 1, -1))


def route(step, me, groups, slots):
    turn, quarter = step // slots, groups // 4
    at_end = (me // quarter) % 3 == 0
    outer = down(groups, 0)
    inner = [
        *down(3 * quarter, quarter), *down(groups, 3 * quarter), *down(quarter, 0)
    ]
    flips = 0
    for at, (far, near) in enumerate(zip(outer, inner)):
        flips = jnp.where(turn == at, jnp.where(at_end, far, near), flips)
    target, bit = 0, 1
    while bit < groups:
        target += (me // bit + flips // bit) % 2 * bit
        bit *= 2
    return target, step % slots


def project_kernel(
    groups, slots, rows_ref, deal_ref, gain_ref, feats_ref, w_ref, keys_ref, values_ref,
    natural, mine, theirs, w_mine, w_give, w_theirs, x_out, x_in, x_scale_out, x_scale_in,
    done, landed, load_sem, w_load_sem, w_give_sem, w_send, w_recv, f_send, f_recv,
    x_send, x_recv, s_send, s_recv, o_send, o_recv, core_sem, x_sem, open_sem,
):
    me = lax.axis_index("gx")
    place = lax.axis_index("gy")
    across = place // 2
    core = place % 2
    other_across, other_core = 1 - across, 1 - core
    core_mate = (me, across * 2 + other_core)
    x_mate = (me, other_across * 2 + core)
    share = w_mine.shape[2]
    total = w_ref.shape[1] // 2
    heads = share // HD
    steps = groups * slots
    leaving = steps - slots

    def columns(block, of_core):
        chip = other_across if block < 2 else across
        first = (block % 2) * total + (chip * 2 + of_core) * share
        return pl.ds(pl.multiple_of(first, 128), share)

    def w_load(b, of_core, into, sem):
        return pltpu.make_async_copy(w_ref.at[:, columns(b, of_core)], into.at[b], sem.at[b])

    loads = [
        pltpu.make_async_copy(
            feats_ref.at[pl.ds(c * groups, groups)], natural[c], load_sem.at[c]
        )
        for c in range(slots)
    ]
    w_loads = [w_load(b, core, w_mine, w_load_sem) for b in range(4)]
    w_gives = [w_load(b, other_core, w_give, w_give_sem) for b in range(4)]
    for copy in (w_gives[0], loads[0], w_gives[1], w_loads[0], *loads[1:], w_loads[1]):
        copy.start()
    for copy in (*w_gives[2:], *w_loads[2:]):
        copy.start()

    barrier = pltpu.get_barrier_semaphore()
    leads = place == 0
    answers = place == 2

    def greet(sem, mate):
        pl.semaphore_signal(sem, inc=1, device_id=mate, device_id_type=MESH)

    @pl.when(core == 0)
    def _():
        greet(barrier, core_mate)
        pl.semaphore_wait(core_sem, 1)

    @pl.when(core == 1)
    def _():
        pl.semaphore_wait(barrier, 1)
        greet(core_sem, core_mate)

    pl.when(leads)(lambda: greet(barrier, x_mate))

    def answer_x():
        pl.semaphore_wait(barrier, 1)
        greet(x_sem, x_mate)
        greet(x_sem, core_mate)

    def meet_x():
        @pl.when(~answers)
        def _():
            pl.semaphore_wait(x_sem, 1)

        @pl.when(leads)
        def _():
            greet(x_sem, core_mate)
            for ahead in range(1, groups):
                greet(barrier, ((me + ahead) % groups, 0))

    def open_deal():
        pl.semaphore_wait(barrier, groups - 1)
        for mate in range(1, 4):
            greet(open_sem, (me, mate))

    w_copies = [
        pltpu.make_async_remote_copy(
            src_ref=w_give.at[b],
            dst_ref=w_theirs.at[b],
            send_sem=w_send.at[b],
            recv_sem=w_recv.at[b],
            device_id=core_mate,
            device_id_type=MESH,
        )
        for b in range(4)
    ]

    def send_weights(b):
        w_gives[b].wait()
        w_copies[b].start()

    def f_copy(k):
        return pltpu.make_async_remote_copy(
            src_ref=mine.at[k], dst_ref=theirs.at[k], send_sem=f_send.at[k],
            recv_sem=f_recv.at[k], device_id=core_mate, device_id_type=MESH,
        )

    def x_copy(b, k):
        return pltpu.make_async_remote_copy(
            src_ref=x_out.at[b, k], dst_ref=x_in.at[b, k], send_sem=x_send.at[b, k],
            recv_sem=x_recv.at[b, k], device_id=x_mate, device_id_type=MESH,
        )

    def s_copy(k):
        return pltpu.make_async_remote_copy(
            src_ref=x_scale_out.at[k], dst_ref=x_scale_in.at[k], send_sem=s_send.at[k],
            recv_sem=s_recv.at[k], device_id=x_mate, device_id_type=MESH,
        )

    def o_copy(b, k, target, landing):
        return pltpu.make_async_remote_copy(
            src_ref=done.at[b, k], dst_ref=landed.at[b, landing], send_sem=o_send.at[b, k],
            recv_sem=o_recv.at[b, landing], device_id=(target, place), device_id_type=MESH,
        )

    def own_column(k):
        target, cls = route(k, me, groups, slots)
        own = 0
        for column in range(groups):
            named = deal_ref[target, cls * groups + column]
            own = jnp.where(named // TPD == me, column, own)
        return own

    def order(k):
        own = own_column(k)
        if isinstance(k, int):
            mine[k] = natural[k % slots][own]
        else:
            for cls in range(slots):

                @pl.when(k % slots == cls)
                def _():
                    mine[k] = natural[cls][own]

        f_copy(k).start()

    send_weights(0)
    loads[0].wait()
    order(0)
    send_weights(1)
    pl.when(answers)(answer_x)
    for copy in loads[1:]:
        copy.wait()
    order(1)
    send_weights(2)
    send_weights(3)
    for k in range(2, AHEAD):
        order(k)
    meet_x()

    def partial(k, block):
        return jnp.dot(
            mine[k], w_mine[block], preferred_element_type=jnp.float32
        ) + jnp.dot(theirs[k], w_theirs[block], preferred_element_type=jnp.float32)

    def weights_here(b):
        w_loads[b].wait()
        w_copies[b].wait_recv()

    def outward(k, first):
        f_copy(k).wait_recv()
        lane = lax.broadcasted_iota(jnp.int32, (TILE, HD), 1)
        peaks = jnp.zeros((TILE, HD), jnp.float32)
        for b in range(2):
            if first:
                weights_here(b)
            sums = partial(k, b)
            for h in range(heads):
                one = sums[:, h * HD : (h + 1) * HD]
                peak = jnp.maximum(jnp.max(jnp.abs(one), axis=-1, keepdims=True), LEAST)
                coded = jnp.round(one * (STEPS / peak)).astype(jnp.int32)
                x_out[b, k, :, h * HD : (h + 1) * HD] = coded.astype(jnp.int16)
                peaks = jnp.where(lane == b * heads + h, peak, peaks)
            if b == 1:
                x_scale_out[k] = jnp.transpose(peaks)[: 2 * heads]
                s_copy(k).start()
            x_copy(b, k).start()

    def finish(k, send):
        target, cls = route(k, me, groups, slots)
        limit = rows_ref[me * TPD + cls * groups + own_column(k)]
        kept = lax.broadcasted_iota(jnp.int32, (TILE, HD), 0) < limit
        for b in range(2):
            part = partial(k, 2 + b)
            if b == 0:
                s_copy(k).wait_recv()
                repeats = HD // (2 * heads)
                peaks = jnp.transpose(jnp.concatenate([x_scale_in[k]] * repeats, axis=0))
            x_copy(b, k).wait_recv()
            for h in range(heads):
                head, at = slice(h * HD, (h + 1) * HD), b * heads + h
                other = x_in[b, k, :, head].astype(jnp.float32)
                one = part[:, head] + other * (peaks[:, at : at + 1] * (1.0 / STEPS))
                if b == 0:
                    mean_square = jnp.mean(one * one, axis=-1, keepdims=True)
                    one = one * lax.rsqrt(mean_square + epsilon) * gain_ref[...]
                done[b, k, :, head] = jnp.where(kept, one, 0.0).astype(jnp.bfloat16)
            if send:
                o_copy(b, k, target, me * slots + cls).start()
            else:
                landed[b, target * slots + cls] = done[b, k]

    def opening(k, carry):
        order(k + AHEAD)
        outward(k, False)
        return carry

    def middle(k, carry):
        @pl.when(k + AHEAD < steps)
        def _():
            order(k + AHEAD)

        outward(k, False)

        @pl.when(~leads & (k == LEAD))
        def _():
            pl.semaphore_wait(open_sem, 1)

        finish(k - LEAD, True)
        return carry

    def closing(k, carry):
        finish(k, True)
        return carry

    outward(0, True)
    order(AHEAD)
    lax.fori_loop(1, LEAD, opening, 0)
    pl.when(leads)(open_deal)
    for b in range(2, 4):
        weights_here(b)
    lax.fori_loop(LEAD, steps, middle, 0)
    lax.fori_loop(steps - LEAD, leaving, closing, 0)
    for c in range(slots):
        finish(leaving + c, False)

    for copy in w_copies:
        copy.wait_send()

    def drain(k, carry):
        f_copy(k).wait_send()
        s_copy(k).wait_send()
        for b in range(2):
            x_copy(b, k).wait_send()
        return carry

    lax.fori_loop(0, steps, drain, 0)

    def drain_out(k, carry):
        target, cls = route(k, me, groups, slots)
        for b in range(2):
            o_copy(b, k, target, me * slots + cls).wait_send()
            o_copy(b, k, target, target * slots + cls).wait_recv()
        return carry

    lax.fori_loop(0, leaving, drain_out, 0)

    def settle(tile, carry):
        landing = deal_ref[me, tile] // TPD * slots + tile // groups
        rows = pl.ds(pl.multiple_of(tile * TILE, TILE), TILE)
        keys_ref[rows, :] = landed[0, landing]
        values_ref[rows, :] = landed[1, landing]
        return carry

    lax.fori_loop(0, TPD, settle, 0)


def store_kernel(keys_ref, values_ref, keys_out, values_out, sem):
    parts = keys_ref.shape[0] // PARTS
    stores = []
    for which, (source, out) in enumerate(((keys_ref, keys_out), (values_ref, values_out))):
        for part in range(PARTS):
            rows = pl.ds(part * parts, parts)
            stores.append(
                pltpu.make_async_copy(source.at[rows], out.at[rows], sem.at[which, part])
            )
            stores[-1].start()
    for copy in stores:
        copy.wait()


def kernel_local(image_feats, w_kv, k_gain, tile_rows, deal):
    groups = lax.axis_size("gx")
    slots = TPD // groups
    width = image_feats.shape[1]
    share = w_kv.shape[1] // 2 // lax.axis_size("gy")
    steps = TPD
    bf16, f32 = jnp.bfloat16, jnp.float32
    smem = pl.BlockSpec(memory_space=pltpu.SMEM)
    anywhere = pl.BlockSpec(memory_space=pl.ANY)
    dma = pltpu.SemaphoreType.DMA

    tiles = pltpu.VMEM((steps, TILE, width), bf16)
    weights = pltpu.VMEM((4, width, share), bf16)
    codes = pltpu.VMEM((2, steps, TILE, share), jnp.int16)
    scales = pltpu.VMEM((steps, 2 * share // HD, HD), f32)
    results = pltpu.VMEM((2, steps, TILE, share), bf16)
    result = pltpu.VMEM((TPD * TILE, share), bf16)
    vmem = pl.BlockSpec(memory_space=pltpu.VMEM)
    results = pl.pallas_call(
        functools.partial(project_kernel, groups, slots),
        out_shape=(result, result),
        in_specs=[smem, smem, vmem, anywhere, anywhere],
        out_specs=(vmem, vmem),
        scratch_shapes=[
            [pltpu.VMEM((groups, TILE, width), bf16)] * slots, tiles, tiles,
            weights, weights, weights, codes, codes, scales, scales,
            results, results, dma((slots,)), dma((4,)), dma((4,)), dma((4,)), dma((4,)),
            dma((steps,)), dma((steps,)), dma((2, steps)), dma((2, steps)),
            dma((steps,)), dma((steps,)), dma((2, steps)), dma((2, steps)),
            *[pltpu.SemaphoreType.REGULAR] * 3,
        ],
        compiler_params=pltpu.CompilerParams(collective_id=0, has_side_effects=True),
        name="project_and_deal",
    )(tile_rows, deal, k_gain.reshape(1, HD), image_feats.reshape(steps, TILE, width), w_kv)
    stored = jax.ShapeDtypeStruct((TPD * TILE, share), bf16)
    return pl.pallas_call(
        store_kernel,
        out_shape=(stored, stored),
        in_specs=[vmem, vmem],
        out_specs=(anywhere, anywhere),
        scratch_shapes=[dma((2, PARTS))],
        name="store_result",
    )(*[pltpu.with_memory_space_constraint(part, pltpu.VMEM) for part in results])


def solution(mesh):
    groups, width_parts = mesh.shape["gx"], mesh.shape["gy"]
    direct = groups % 4 == 0 and TPD % groups == 0 and width_parts == 4
    local = kernel_local if direct else plain_local
    placed = (P("gx", "gy"), P("gy", None), P(), P(), P())
    return jax.shard_map(
        local, mesh=mesh, in_specs=placed, out_specs=(P("gx", "gy"), P("gx", "gy")), check_vma=False
    )
```

```python
import functools

import jax
import jax.numpy as jnp
from jax import lax
from jax.experimental import pallas as pl
from jax.experimental.pallas import tpu as pltpu
from jax.sharding import PartitionSpec as P

HD = 128
TILE = 128
TPD = 16


epsilon = 1e-05


def plain_local(image_feats, w_kv, k_gain, tile_rows, deal):
    local_width = image_feats.shape[1]
    groups = lax.axis_size("gx")
    own_index = lax.axis_index("gx")
    slots = max(1, TPD // groups)
    wanted = lax.dynamic_index_in_dim(deal, own_index, 0, keepdims=False)
    slot_index = jnp.arange(TPD, dtype=jnp.int32)
    slot_class = slot_index // groups
    places = jnp.arange(slots, dtype=jnp.int32)
    class_match = slot_class[None, :] == places[:, None]
    own_tiles = own_index * TPD + slot_index
    sending = deal == own_tiles[None, :]
    send_select = (sending[:, None, :] & class_match[None, :, :]).astype(jnp.bfloat16)
    blocks = image_feats.reshape(TPD, TILE, local_width)
    outgoing = jnp.einsum(
        "dcs,str->dctr", send_select, blocks, preferred_element_type=jnp.float32
    ).astype(jnp.bfloat16)
    incoming = lax.all_to_all(outgoing, "gx", split_axis=0, concat_axis=0, tiled=True)
    sources = jnp.arange(groups, dtype=jnp.int32)
    from_source = (wanted // TPD)[:, None] == sources[None, :]
    take_select = (from_source[:, :, None] & class_match.T[:, None, :]).astype(jnp.bfloat16)
    dealt_tiles = jnp.einsum(
        "snc,nctr->str", take_select, incoming, preferred_element_type=jnp.float32
    ).astype(jnp.bfloat16)
    row_count = TPD * TILE
    dealt_rows = dealt_tiles.reshape(row_count, local_width)
    total_kv = w_kv.shape[1] // 2
    partial_value = jnp.dot(dealt_rows, w_kv, preferred_element_type=jnp.float32)
    projected = lax.psum_scatter(
        partial_value.reshape(row_count, 2, total_kv), "gy", scatter_dimension=2, tiled=True
    )
    share_cols = projected.shape[2]
    key_pre = projected[:, 0, :].reshape(row_count, share_cols // HD, HD)
    value_pre = projected[:, 1, :]
    mean_square = jnp.mean(key_pre * key_pre, axis=-1, keepdims=True)
    normed = (key_pre * lax.rsqrt(mean_square + epsilon) * k_gain).reshape(row_count, share_cols)
    all_tiles = jnp.arange(tile_rows.shape[0], dtype=jnp.int32)
    limits = jnp.sum(
        jnp.where(wanted[:, None] == all_tiles[None, :], tile_rows[None, :], 0), axis=1
    )
    position = jnp.arange(TILE, dtype=jnp.int32)
    valid_rows = (position[None, :] < limits[:, None]).reshape(row_count, 1)
    keys_out = jnp.where(valid_rows, normed, 0.0).astype(jnp.bfloat16)
    values_out = jnp.where(valid_rows, value_pre, 0.0).astype(jnp.bfloat16)
    return (keys_out, values_out)


MESH = pl.DeviceIdType.MESH
STEPS = 32767.0
LEAST = 1e-30
AHEAD = 4
LEAD = 2
PARTS = 4


def down(top, bottom):
    return list(range(top - 1, bottom - 1, -1))


def route(step, me, groups, slots):
    turn, quarter = step // slots, groups // 4
    at_end = (me // quarter) % 3 == 0
    outer = down(groups, 0)
    inner = [
        *down(3 * quarter, quarter), *down(groups, 3 * quarter), *down(quarter, 0)
    ]
    flips = 0
    for at, (far, near) in enumerate(zip(outer, inner)):
        flips = jnp.where(turn == at, jnp.where(at_end, far, near), flips)
    target, bit = 0, 1
    while bit < groups:
        target += (me // bit + flips // bit) % 2 * bit
        bit *= 2
    return target, step % slots


def project_kernel(
    groups, slots, rows_ref, deal_ref, gain_ref, feats_ref, w_ref, keys_ref, values_ref,
    natural, mine, theirs, w_mine, w_give, w_theirs, x_out, x_in, x_scale_out, x_scale_in,
    done, landed, load_sem, w_load_sem, w_give_sem, w_send, w_recv, f_send, f_recv,
    x_send, x_recv, s_send, s_recv, o_send, o_recv, core_sem, x_sem, open_sem,
):
    me = lax.axis_index("gx")
    place = lax.axis_index("gy")
    across = place // 2
    core = place % 2
    other_across, other_core = 1 - across, 1 - core
    core_mate = (me, across * 2 + other_core)
    x_mate = (me, other_across * 2 + core)
    share = w_mine.shape[2]
    total = w_ref.shape[1] // 2
    heads = share // HD
    steps = groups * slots
    leaving = steps - slots

    def columns(block, of_core):
        chip = other_across if block < 2 else across
        first = (block % 2) * total + (chip * 2 + of_core) * share
        return pl.ds(pl.multiple_of(first, 128), share)

    def w_load(b, of_core, into, sem):
        return pltpu.make_async_copy(w_ref.at[:, columns(b, of_core)], into.at[b], sem.at[b])

    loads = [
        pltpu.make_async_copy(
            feats_ref.at[pl.ds(c * groups, groups)], natural[c], load_sem.at[c]
        )
        for c in range(slots)
    ]
    w_loads = [w_load(b, core, w_mine, w_load_sem) for b in range(4)]
    w_gives = [w_load(b, other_core, w_give, w_give_sem) for b in range(4)]
    for copy in (w_gives[0], loads[0], w_gives[1], w_loads[0], *loads[1:], w_loads[1]):
        copy.start()
    for copy in (*w_gives[2:], *w_loads[2:]):
        copy.start()

    barrier = pltpu.get_barrier_semaphore()
    leads = place == 0
    answers = place == 2

    def greet(sem, mate):
        pl.semaphore_signal(sem, inc=1, device_id=mate, device_id_type=MESH)

    @pl.when(core == 0)
    def _():
        greet(barrier, core_mate)
        pl.semaphore_wait(core_sem, 1)

    @pl.when(core == 1)
    def _():
        pl.semaphore_wait(barrier, 1)
        greet(core_sem, core_mate)

    pl.when(leads)(lambda: greet(barrier, x_mate))

    def answer_x():
        pl.semaphore_wait(barrier, 1)
        greet(x_sem, x_mate)
        greet(x_sem, core_mate)

    def meet_x():
        @pl.when(~answers)
        def _():
            pl.semaphore_wait(x_sem, 1)

        @pl.when(leads)
        def _():
            greet(x_sem, core_mate)
            for ahead in range(1, groups):
                greet(barrier, ((me + ahead) % groups, 0))

    def open_deal():
        pl.semaphore_wait(barrier, groups - 1)
        for mate in range(1, 4):
            greet(open_sem, (me, mate))

    w_copies = [
        pltpu.make_async_remote_copy(
            src_ref=w_give.at[b],
            dst_ref=w_theirs.at[b],
            send_sem=w_send.at[b],
            recv_sem=w_recv.at[b],
            device_id=core_mate,
            device_id_type=MESH,
        )
        for b in range(4)
    ]

    def send_weights(b):
        w_gives[b].wait()
        w_copies[b].start()

    def f_copy(k):
        return pltpu.make_async_remote_copy(
            src_ref=mine.at[k], dst_ref=theirs.at[k], send_sem=f_send.at[k],
            recv_sem=f_recv.at[k], device_id=core_mate, device_id_type=MESH,
        )

    def x_copy(b, k):
        return pltpu.make_async_remote_copy(
            src_ref=x_out.at[b, k], dst_ref=x_in.at[b, k], send_sem=x_send.at[b, k],
            recv_sem=x_recv.at[b, k], device_id=x_mate, device_id_type=MESH,
        )

    def s_copy(k):
        return pltpu.make_async_remote_copy(
            src_ref=x_scale_out.at[k], dst_ref=x_scale_in.at[k], send_sem=s_send.at[k],
            recv_sem=s_recv.at[k], device_id=x_mate, device_id_type=MESH,
        )

    def o_copy(b, k, target, landing):
        return pltpu.make_async_remote_copy(
            src_ref=done.at[b, k], dst_ref=landed.at[b, landing], send_sem=o_send.at[b, k],
            recv_sem=o_recv.at[b, landing], device_id=(target, place), device_id_type=MESH,
        )

    def own_column(k):
        target, cls = route(k, me, groups, slots)
        own = 0
        for column in range(groups):
            named = deal_ref[target, cls * groups + column]
            own = jnp.where(named // TPD == me, column, own)
        return own

    def order(k):
        own = own_column(k)
        if isinstance(k, int):
            mine[k] = natural[k % slots][own]
        else:
            for cls in range(slots):

                @pl.when(k % slots == cls)
                def _():
                    mine[k] = natural[cls][own]

        f_copy(k).start()

    send_weights(0)
    loads[0].wait()
    order(0)
    send_weights(1)
    pl.when(answers)(answer_x)
    for copy in loads[1:]:
        copy.wait()
    order(1)
    send_weights(2)
    send_weights(3)
    for k in range(2, AHEAD):
        order(k)
    meet_x()

    def partial(k, block):
        return jnp.dot(
            mine[k], w_mine[block], preferred_element_type=jnp.float32
        ) + jnp.dot(theirs[k], w_theirs[block], preferred_element_type=jnp.float32)

    def weights_here(b):
        w_loads[b].wait()
        w_copies[b].wait_recv()

    def outward(k, first):
        f_copy(k).wait_recv()
        lane = lax.broadcasted_iota(jnp.int32, (TILE, HD), 1)
        peaks = jnp.zeros((TILE, HD), jnp.float32)
        for b in range(2):
            if first:
                weights_here(b)
            sums = partial(k, b)
            for h in range(heads):
                one = sums[:, h * HD : (h + 1) * HD]
                peak = jnp.maximum(jnp.max(jnp.abs(one), axis=-1, keepdims=True), LEAST)
                coded = jnp.round(one * (STEPS / peak)).astype(jnp.int32)
                x_out[b, k, :, h * HD : (h + 1) * HD] = coded.astype(jnp.int16)
                peaks = jnp.where(lane == b * heads + h, peak, peaks)
            if b == 1:
                x_scale_out[k] = jnp.transpose(peaks)[: 2 * heads]
                s_copy(k).start()
            x_copy(b, k).start()

    def finish(k, send):
        target, cls = route(k, me, groups, slots)
        limit = rows_ref[me * TPD + cls * groups + own_column(k)]
        kept = lax.broadcasted_iota(jnp.int32, (TILE, HD), 0) < limit
        for b in range(2):
            part = partial(k, 2 + b)
            if b == 0:
                s_copy(k).wait_recv()
                repeats = HD // (2 * heads)
                peaks = jnp.transpose(jnp.concatenate([x_scale_in[k]] * repeats, axis=0))
            x_copy(b, k).wait_recv()
            for h in range(heads):
                head, at = slice(h * HD, (h + 1) * HD), b * heads + h
                other = x_in[b, k, :, head].astype(jnp.float32)
                one = part[:, head] + other * (peaks[:, at : at + 1] * (1.0 / STEPS))
                if b == 0:
                    mean_square = jnp.mean(one * one, axis=-1, keepdims=True)
                    one = one * lax.rsqrt(mean_square + epsilon) * gain_ref[...]
                done[b, k, :, head] = jnp.where(kept, one, 0.0).astype(jnp.bfloat16)
            if send:
                o_copy(b, k, target, me * slots + cls).start()
            else:
                landed[b, target * slots + cls] = done[b, k]

    def opening(k, carry):
        order(k + AHEAD)
        outward(k, False)
        return carry

    def middle(k, carry):
        @pl.when(k + AHEAD < steps)
        def _():
            order(k + AHEAD)

        outward(k, False)

        @pl.when(~leads & (k == LEAD))
        def _():
            pl.semaphore_wait(open_sem, 1)

        finish(k - LEAD, True)
        return carry

    def closing(k, carry):
        finish(k, True)
        return carry

    outward(0, True)
    order(AHEAD)
    lax.fori_loop(1, LEAD, opening, 0)
    pl.when(leads)(open_deal)
    for b in range(2, 4):
        weights_here(b)
    lax.fori_loop(LEAD, steps, middle, 0)
    lax.fori_loop(steps - LEAD, leaving, closing, 0)
    for copy in w_copies:
        copy.wait_send()

    def sent(k, carry):
        f_copy(k).wait_send()
        s_copy(k).wait_send()
        for b in range(2):
            x_copy(b, k).wait_send()
        return carry

    def dealt(k, carry):
        for b in range(2):
            o_copy(b, k, me, 0).wait_send()
        return carry

    def arrived(ahead, carry):
        source = (me + ahead) % groups
        for cls in range(slots):
            for b in range(2):
                o_copy(b, 0, source, source * slots + cls).wait_recv()
        return carry

    lax.fori_loop(0, leaving, sent, 0)
    for c in range(slots):
        finish(leaving + c, False)
    lax.fori_loop(leaving, steps, sent, 0)
    lax.fori_loop(0, leaving, dealt, 0)
    lax.fori_loop(1, groups, arrived, 0)

    def settle(tile, carry):
        landing = deal_ref[me, tile] // TPD * slots + tile // groups
        rows = pl.ds(pl.multiple_of(tile * TILE, TILE), TILE)
        keys_ref[rows, :] = landed[0, landing]
        values_ref[rows, :] = landed[1, landing]
        return carry

    lax.fori_loop(0, TPD, settle, 0, unroll=16)


def store_kernel(keys_ref, values_ref, keys_out, values_out, sem):
    parts = keys_ref.shape[0] // PARTS
    stores = []
    for which, (source, out) in enumerate(((keys_ref, keys_out), (values_ref, values_out))):
        for part in range(PARTS):
            rows = pl.ds(part * parts, parts)
            stores.append(
                pltpu.make_async_copy(source.at[rows], out.at[rows], sem.at[which, part])
            )
            stores[-1].start()
    for copy in stores:
        copy.wait()


def kernel_local(image_feats, w_kv, k_gain, tile_rows, deal):
    groups = lax.axis_size("gx")
    slots = TPD // groups
    width = image_feats.shape[1]
    share = w_kv.shape[1] // 2 // lax.axis_size("gy")
    steps = TPD
    bf16, f32 = jnp.bfloat16, jnp.float32
    smem = pl.BlockSpec(memory_space=pltpu.SMEM)
    anywhere = pl.BlockSpec(memory_space=pl.ANY)
    dma = pltpu.SemaphoreType.DMA

    tiles = pltpu.VMEM((steps, TILE, width), bf16)
    weights = pltpu.VMEM((4, width, share), bf16)
    codes = pltpu.VMEM((2, steps, TILE, share), jnp.int16)
    scales = pltpu.VMEM((steps, 2 * share // HD, HD), f32)
    results = pltpu.VMEM((2, steps, TILE, share), bf16)
    result = pltpu.VMEM((TPD * TILE, share), bf16)
    vmem = pl.BlockSpec(memory_space=pltpu.VMEM)
    results = pl.pallas_call(
        functools.partial(project_kernel, groups, slots),
        out_shape=(result, result),
        in_specs=[smem, smem, vmem, anywhere, anywhere],
        out_specs=(vmem, vmem),
        scratch_shapes=[
            [pltpu.VMEM((groups, TILE, width), bf16)] * slots, tiles, tiles,
            weights, weights, weights, codes, codes, scales, scales,
            results, results, dma((slots,)), dma((4,)), dma((4,)), dma((4,)), dma((4,)),
            dma((steps,)), dma((steps,)), dma((2, steps)), dma((2, steps)),
            dma((steps,)), dma((steps,)), dma((2, steps)), dma((2, steps)),
            *[pltpu.SemaphoreType.REGULAR] * 3,
        ],
        compiler_params=pltpu.CompilerParams(collective_id=0, has_side_effects=True),
        name="project_and_deal",
    )(tile_rows, deal, k_gain.reshape(1, HD), image_feats.reshape(steps, TILE, width), w_kv)
    stored = jax.ShapeDtypeStruct((TPD * TILE, share), bf16)
    return pl.pallas_call(
        store_kernel,
        out_shape=(stored, stored),
        in_specs=[vmem, vmem],
        out_specs=(anywhere, anywhere),
        scratch_shapes=[dma((2, PARTS))],
        name="store_result",
    )(*[pltpu.with_memory_space_constraint(part, pltpu.VMEM) for part in results])


def solution(mesh):
    groups, width_parts = mesh.shape["gx"], mesh.shape["gy"]
    direct = groups % 4 == 0 and TPD % groups == 0 and width_parts == 4
    local = kernel_local if direct else plain_local
    placed = (P("gx", "gy"), P("gy", None), P(), P(), P())
    return jax.shard_map(
        local, mesh=mesh, in_specs=placed, out_specs=(P("gx", "gy"), P("gx", "gy")), check_vma=False
    )
```

```python
import functools

import jax
import jax.numpy as jnp
from jax import lax
from jax.experimental import pallas as pl
from jax.experimental.pallas import tpu as pltpu
from jax.sharding import PartitionSpec as P

HD = 128
TILE = 128
TPD = 16


epsilon = 1e-05


def plain_local(image_feats, w_kv, k_gain, tile_rows, deal):
    local_width = image_feats.shape[1]
    groups = lax.axis_size("gx")
    own_index = lax.axis_index("gx")
    slots = max(1, TPD // groups)
    wanted = lax.dynamic_index_in_dim(deal, own_index, 0, keepdims=False)
    slot_index = jnp.arange(TPD, dtype=jnp.int32)
    slot_class = slot_index // groups
    places = jnp.arange(slots, dtype=jnp.int32)
    class_match = slot_class[None, :] == places[:, None]
    own_tiles = own_index * TPD + slot_index
    sending = deal == own_tiles[None, :]
    send_select = (sending[:, None, :] & class_match[None, :, :]).astype(jnp.bfloat16)
    blocks = image_feats.reshape(TPD, TILE, local_width)
    outgoing = jnp.einsum(
        "dcs,str->dctr", send_select, blocks, preferred_element_type=jnp.float32
    ).astype(jnp.bfloat16)
    incoming = lax.all_to_all(outgoing, "gx", split_axis=0, concat_axis=0, tiled=True)
    sources = jnp.arange(groups, dtype=jnp.int32)
    from_source = (wanted // TPD)[:, None] == sources[None, :]
    take_select = (from_source[:, :, None] & class_match.T[:, None, :]).astype(jnp.bfloat16)
    dealt_tiles = jnp.einsum(
        "snc,nctr->str", take_select, incoming, preferred_element_type=jnp.float32
    ).astype(jnp.bfloat16)
    row_count = TPD * TILE
    dealt_rows = dealt_tiles.reshape(row_count, local_width)
    total_kv = w_kv.shape[1] // 2
    partial_value = jnp.dot(dealt_rows, w_kv, preferred_element_type=jnp.float32)
    projected = lax.psum_scatter(
        partial_value.reshape(row_count, 2, total_kv), "gy", scatter_dimension=2, tiled=True
    )
    share_cols = projected.shape[2]
    key_pre = projected[:, 0, :].reshape(row_count, share_cols // HD, HD)
    value_pre = projected[:, 1, :]
    mean_square = jnp.mean(key_pre * key_pre, axis=-1, keepdims=True)
    normed = (key_pre * lax.rsqrt(mean_square + epsilon) * k_gain).reshape(row_count, share_cols)
    all_tiles = jnp.arange(tile_rows.shape[0], dtype=jnp.int32)
    limits = jnp.sum(
        jnp.where(wanted[:, None] == all_tiles[None, :], tile_rows[None, :], 0), axis=1
    )
    position = jnp.arange(TILE, dtype=jnp.int32)
    valid_rows = (position[None, :] < limits[:, None]).reshape(row_count, 1)
    keys_out = jnp.where(valid_rows, normed, 0.0).astype(jnp.bfloat16)
    values_out = jnp.where(valid_rows, value_pre, 0.0).astype(jnp.bfloat16)
    return (keys_out, values_out)


MESH = pl.DeviceIdType.MESH
STEPS = 32767.0
LEAST = 1e-30
AHEAD = 4
LEAD = 2
PARTS = 4


def down(top, bottom):
    return list(range(top - 1, bottom - 1, -1))


def route(step, me, groups, slots):
    turn, quarter = step // slots, groups // 4
    at_end = (me // quarter) % 3 == 0
    outer = down(groups, 0)
    inner = [
        *down(3 * quarter, quarter), *down(groups, 3 * quarter), *down(quarter, 0)
    ]
    flips = 0
    for at, (far, near) in enumerate(zip(outer, inner)):
        flips = jnp.where(turn == at, jnp.where(at_end, far, near), flips)
    target, bit = 0, 1
    while bit < groups:
        target += (me // bit + flips // bit) % 2 * bit
        bit *= 2
    return target, step % slots


def project_kernel(
    groups, slots, rows_ref, deal_ref, gain_ref, feats_ref, w_ref, keys_ref, values_ref,
    natural, mine, theirs, w_mine, w_give, w_theirs, x_out, x_in, x_scale_out, x_scale_in,
    done, landed, load_sem, w_load_sem, w_give_sem, w_send, w_recv, f_send, f_recv,
    x_send, x_recv, s_send, s_recv, o_send, o_recv, core_sem, x_sem, open_sem,
):
    me = lax.axis_index("gx")
    place = lax.axis_index("gy")
    across = place // 2
    core = place % 2
    other_across, other_core = 1 - across, 1 - core
    core_mate = (me, across * 2 + other_core)
    x_mate = (me, other_across * 2 + core)
    share = w_mine.shape[2]
    total = w_ref.shape[1] // 2
    heads = share // HD
    steps = groups * slots
    leaving = steps - slots

    def columns(block, of_core):
        chip = other_across if block < 2 else across
        first = (block % 2) * total + (chip * 2 + of_core) * share
        return pl.ds(pl.multiple_of(first, 128), share)

    def w_load(b, of_core, into, sem):
        return pltpu.make_async_copy(w_ref.at[:, columns(b, of_core)], into.at[b], sem.at[b])

    loads = [
        pltpu.make_async_copy(
            feats_ref.at[pl.ds(c * groups, groups)], natural[c], load_sem.at[c]
        )
        for c in range(slots)
    ]
    w_loads = [w_load(b, core, w_mine, w_load_sem) for b in range(4)]
    w_gives = [w_load(b, other_core, w_give, w_give_sem) for b in range(4)]
    for copy in (loads[0], w_gives[0], w_gives[1], w_loads[0], *loads[1:], w_loads[1]):
        copy.start()
    for copy in (*w_gives[2:], *w_loads[2:]):
        copy.start()

    barrier = pltpu.get_barrier_semaphore()
    leads = place == 0
    answers = place == 2

    def greet(sem, mate):
        pl.semaphore_signal(sem, inc=1, device_id=mate, device_id_type=MESH)

    @pl.when(core == 0)
    def _():
        greet(barrier, core_mate)
        pl.semaphore_wait(core_sem, 1)

    @pl.when(core == 1)
    def _():
        pl.semaphore_wait(barrier, 1)
        greet(core_sem, core_mate)

    pl.when(leads)(lambda: greet(barrier, x_mate))

    def answer_x():
        pl.semaphore_wait(barrier, 1)
        greet(x_sem, x_mate)
        greet(x_sem, core_mate)

    def meet_x():
        @pl.when(~answers)
        def _():
            pl.semaphore_wait(x_sem, 1)

        @pl.when(leads)
        def _():
            greet(x_sem, core_mate)
            for ahead in range(1, groups):
                greet(barrier, ((me + ahead) % groups, 0))

    def open_deal():
        pl.semaphore_wait(barrier, groups - 1)
        for mate in range(1, 4):
            greet(open_sem, (me, mate))

    w_copies = [
        pltpu.make_async_remote_copy(
            src_ref=w_give.at[b],
            dst_ref=w_theirs.at[b],
            send_sem=w_send.at[b],
            recv_sem=w_recv.at[b],
            device_id=core_mate,
            device_id_type=MESH,
        )
        for b in range(4)
    ]

    def send_weights(b):
        w_gives[b].wait()
        w_copies[b].start()

    def f_copy(k):
        return pltpu.make_async_remote_copy(
            src_ref=mine.at[k], dst_ref=theirs.at[k], send_sem=f_send.at[k],
            recv_sem=f_recv.at[k], device_id=core_mate, device_id_type=MESH,
        )

    def x_copy(b, k):
        return pltpu.make_async_remote_copy(
            src_ref=x_out.at[b, k], dst_ref=x_in.at[b, k], send_sem=x_send.at[b, k],
            recv_sem=x_recv.at[b, k], device_id=x_mate, device_id_type=MESH,
        )

    def s_copy(k):
        return pltpu.make_async_remote_copy(
            src_ref=x_scale_out.at[k], dst_ref=x_scale_in.at[k], send_sem=s_send.at[k],
            recv_sem=s_recv.at[k], device_id=x_mate, device_id_type=MESH,
        )

    def o_copy(b, k, target, landing):
        return pltpu.make_async_remote_copy(
            src_ref=done.at[b, k], dst_ref=landed.at[b, landing], send_sem=o_send.at[b, k],
            recv_sem=o_recv.at[b, landing], device_id=(target, place), device_id_type=MESH,
        )

    def own_column(k):
        target, cls = route(k, me, groups, slots)
        own = 0
        for column in range(groups):
            named = deal_ref[target, cls * groups + column]
            own = jnp.where(named // TPD == me, column, own)
        return own

    def order(k):
        own = own_column(k)
        if isinstance(k, int):
            mine[k] = natural[k % slots][own]
        else:
            for cls in range(slots):

                @pl.when(k % slots == cls)
                def _():
                    mine[k] = natural[cls][own]

        f_copy(k).start()

    send_weights(0)
    loads[0].wait()
    order(0)
    send_weights(1)
    pl.when(answers)(answer_x)
    for copy in loads[1:]:
        copy.wait()
    order(1)
    send_weights(2)
    send_weights(3)
    for k in range(2, AHEAD):
        order(k)
    meet_x()

    def partial(k, block):
        return jnp.dot(
            mine[k], w_mine[block], preferred_element_type=jnp.float32
        ) + jnp.dot(theirs[k], w_theirs[block], preferred_element_type=jnp.float32)

    def weights_here(b):
        w_loads[b].wait()
        w_copies[b].wait_recv()

    def outward(k, first):
        f_copy(k).wait_recv()
        lane = lax.broadcasted_iota(jnp.int32, (TILE, HD), 1)
        peaks = jnp.zeros((TILE, HD), jnp.float32)
        for b in range(2):
            if first:
                weights_here(b)
            sums = partial(k, b)
            for h in range(heads):
                one = sums[:, h * HD : (h + 1) * HD]
                peak = jnp.maximum(jnp.max(jnp.abs(one), axis=-1, keepdims=True), LEAST)
                coded = jnp.round(one * (STEPS / peak)).astype(jnp.int32)
                x_out[b, k, :, h * HD : (h + 1) * HD] = coded.astype(jnp.int16)
                peaks = jnp.where(lane == b * heads + h, peak, peaks)
            if b == 1:
                x_scale_out[k] = jnp.transpose(peaks)[: 2 * heads]
                s_copy(k).start()
            x_copy(b, k).start()

    def finish(k, send):
        target, cls = route(k, me, groups, slots)
        limit = rows_ref[me * TPD + cls * groups + own_column(k)]
        kept = lax.broadcasted_iota(jnp.int32, (TILE, HD), 0) < limit
        for b in range(2):
            part = partial(k, 2 + b)
            if b == 0:
                s_copy(k).wait_recv()
                repeats = HD // (2 * heads)
                peaks = jnp.transpose(jnp.concatenate([x_scale_in[k]] * repeats, axis=0))
            x_copy(b, k).wait_recv()
            for h in range(heads):
                head, at = slice(h * HD, (h + 1) * HD), b * heads + h
                other = x_in[b, k, :, head].astype(jnp.float32)
                one = part[:, head] + other * (peaks[:, at : at + 1] * (1.0 / STEPS))
                if b == 0:
                    mean_square = jnp.mean(one * one, axis=-1, keepdims=True)
                    one = one * lax.rsqrt(mean_square + epsilon) * gain_ref[...]
                done[b, k, :, head] = jnp.where(kept, one, 0.0).astype(jnp.bfloat16)
            if send:
                o_copy(b, k, target, me * slots + cls).start()
            else:
                landed[b, target * slots + cls] = done[b, k]

    def opening(k, carry):
        order(k + AHEAD)
        outward(k, False)
        return carry

    def middle(k, carry):
        @pl.when(k + AHEAD < steps)
        def _():
            order(k + AHEAD)

        @pl.when(~leads & (k == LEAD))
        def _():
            pl.semaphore_wait(open_sem, 1)

        finish(k - LEAD, True)
        outward(k, False)
        return carry

    def closing(k, carry):
        finish(k, True)
        return carry

    outward(0, True)
    order(AHEAD)
    lax.fori_loop(1, LEAD, opening, 0)
    pl.when(leads)(open_deal)
    for b in range(2, 4):
        weights_here(b)
    lax.fori_loop(LEAD, steps, middle, 0)
    lax.fori_loop(steps - LEAD, leaving, closing, 0)
    for copy in w_copies:
        copy.wait_send()

    def sent(k, carry):
        f_copy(k).wait_send()
        s_copy(k).wait_send()
        for b in range(2):
            x_copy(b, k).wait_send()
        return carry

    def dealt(k, carry):
        for b in range(2):
            o_copy(b, k, me, 0).wait_send()
        return carry

    def arrived(ahead, carry):
        source = (me + ahead) % groups
        for cls in range(slots):
            for b in range(2):
                o_copy(b, 0, source, source * slots + cls).wait_recv()
        return carry

    lax.fori_loop(0, leaving, sent, 0)
    for c in range(slots):
        finish(leaving + c, False)
    lax.fori_loop(leaving, steps, sent, 0)
    lax.fori_loop(0, leaving, dealt, 0)
    lax.fori_loop(1, groups, arrived, 0)

    def settle(tile, carry):
        landing = deal_ref[me, tile] // TPD * slots + tile // groups
        rows = pl.ds(pl.multiple_of(tile * TILE, TILE), TILE)
        keys_ref[rows, :] = landed[0, landing]
        values_ref[rows, :] = landed[1, landing]
        return carry

    lax.fori_loop(0, TPD, settle, 0, unroll=16)


def store_kernel(keys_ref, values_ref, keys_out, values_out, sem):
    parts = keys_ref.shape[0] // PARTS
    stores = []
    for which, (source, out) in enumerate(((keys_ref, keys_out), (values_ref, values_out))):
        for part in range(PARTS):
            rows = pl.ds(part * parts, parts)
            stores.append(
                pltpu.make_async_copy(source.at[rows], out.at[rows], sem.at[which, part])
            )
            stores[-1].start()
    for copy in stores:
        copy.wait()


def kernel_local(image_feats, w_kv, k_gain, tile_rows, deal):
    groups = lax.axis_size("gx")
    slots = TPD // groups
    width = image_feats.shape[1]
    share = w_kv.shape[1] // 2 // lax.axis_size("gy")
    steps = TPD
    bf16, f32 = jnp.bfloat16, jnp.float32
    smem = pl.BlockSpec(memory_space=pltpu.SMEM)
    anywhere = pl.BlockSpec(memory_space=pl.ANY)
    dma = pltpu.SemaphoreType.DMA

    tiles = pltpu.VMEM((steps, TILE, width), bf16)
    weights = pltpu.VMEM((4, width, share), bf16)
    codes = pltpu.VMEM((2, steps, TILE, share), jnp.int16)
    scales = pltpu.VMEM((steps, 2 * share // HD, HD), f32)
    results = pltpu.VMEM((2, steps, TILE, share), bf16)
    result = pltpu.VMEM((TPD * TILE, share), bf16)
    vmem = pl.BlockSpec(memory_space=pltpu.VMEM)
    results = pl.pallas_call(
        functools.partial(project_kernel, groups, slots),
        out_shape=(result, result),
        in_specs=[smem, smem, vmem, anywhere, anywhere],
        out_specs=(vmem, vmem),
        scratch_shapes=[
            [pltpu.VMEM((groups, TILE, width), bf16)] * slots, tiles, tiles,
            weights, weights, weights, codes, codes, scales, scales,
            results, results, dma((slots,)), dma((4,)), dma((4,)), dma((4,)), dma((4,)),
            dma((steps,)), dma((steps,)), dma((2, steps)), dma((2, steps)),
            dma((steps,)), dma((steps,)), dma((2, steps)), dma((2, steps)),
            *[pltpu.SemaphoreType.REGULAR] * 3,
        ],
        compiler_params=pltpu.CompilerParams(collective_id=0, has_side_effects=True),
        name="project_and_deal",
    )(tile_rows, deal, k_gain.reshape(1, HD), image_feats.reshape(steps, TILE, width), w_kv)
    stored = jax.ShapeDtypeStruct((TPD * TILE, share), bf16)
    return pl.pallas_call(
        store_kernel,
        out_shape=(stored, stored),
        in_specs=[vmem, vmem],
        out_specs=(anywhere, anywhere),
        scratch_shapes=[dma((2, PARTS))],
        name="store_result",
    )(*[pltpu.with_memory_space_constraint(part, pltpu.VMEM) for part in results])


def solution(mesh):
    groups, width_parts = mesh.shape["gx"], mesh.shape["gy"]
    direct = groups % 4 == 0 and TPD % groups == 0 and width_parts == 4
    local = kernel_local if direct else plain_local
    placed = (P("gx", "gy"), P("gy", None), P(), P(), P())
    return jax.shard_map(
        local, mesh=mesh, in_specs=placed, out_specs=(P("gx", "gy"), P("gx", "gy")), check_vma=False
    )
```

```python
import functools

import jax
import jax.numpy as jnp
from jax import lax
from jax.experimental import pallas as pl
from jax.experimental.pallas import tpu as pltpu
from jax.sharding import PartitionSpec as P

HD = 128
TILE = 128
TPD = 16


epsilon = 1e-05


def plain_local(image_feats, w_kv, k_gain, tile_rows, deal):
    local_width = image_feats.shape[1]
    groups = lax.axis_size("gx")
    own_index = lax.axis_index("gx")
    slots = max(1, TPD // groups)
    wanted = lax.dynamic_index_in_dim(deal, own_index, 0, keepdims=False)
    slot_index = jnp.arange(TPD, dtype=jnp.int32)
    slot_class = slot_index // groups
    places = jnp.arange(slots, dtype=jnp.int32)
    class_match = slot_class[None, :] == places[:, None]
    own_tiles = own_index * TPD + slot_index
    sending = deal == own_tiles[None, :]
    send_select = (sending[:, None, :] & class_match[None, :, :]).astype(jnp.bfloat16)
    blocks = image_feats.reshape(TPD, TILE, local_width)
    outgoing = jnp.einsum(
        "dcs,str->dctr", send_select, blocks, preferred_element_type=jnp.float32
    ).astype(jnp.bfloat16)
    incoming = lax.all_to_all(outgoing, "gx", split_axis=0, concat_axis=0, tiled=True)
    sources = jnp.arange(groups, dtype=jnp.int32)
    from_source = (wanted // TPD)[:, None] == sources[None, :]
    take_select = (from_source[:, :, None] & class_match.T[:, None, :]).astype(jnp.bfloat16)
    dealt_tiles = jnp.einsum(
        "snc,nctr->str", take_select, incoming, preferred_element_type=jnp.float32
    ).astype(jnp.bfloat16)
    row_count = TPD * TILE
    dealt_rows = dealt_tiles.reshape(row_count, local_width)
    total_kv = w_kv.shape[1] // 2
    partial_value = jnp.dot(dealt_rows, w_kv, preferred_element_type=jnp.float32)
    projected = lax.psum_scatter(
        partial_value.reshape(row_count, 2, total_kv), "gy", scatter_dimension=2, tiled=True
    )
    share_cols = projected.shape[2]
    key_pre = projected[:, 0, :].reshape(row_count, share_cols // HD, HD)
    value_pre = projected[:, 1, :]
    mean_square = jnp.mean(key_pre * key_pre, axis=-1, keepdims=True)
    normed = (key_pre * lax.rsqrt(mean_square + epsilon) * k_gain).reshape(row_count, share_cols)
    all_tiles = jnp.arange(tile_rows.shape[0], dtype=jnp.int32)
    limits = jnp.sum(
        jnp.where(wanted[:, None] == all_tiles[None, :], tile_rows[None, :], 0), axis=1
    )
    position = jnp.arange(TILE, dtype=jnp.int32)
    valid_rows = (position[None, :] < limits[:, None]).reshape(row_count, 1)
    keys_out = jnp.where(valid_rows, normed, 0.0).astype(jnp.bfloat16)
    values_out = jnp.where(valid_rows, value_pre, 0.0).astype(jnp.bfloat16)
    return (keys_out, values_out)


MESH = pl.DeviceIdType.MESH
STEPS = 32767.0
LEAST = 1e-30
AHEAD = 2
LEAD = 2
PARTS = 4


def down(top, bottom):
    return list(range(top - 1, bottom - 1, -1))


def route(step, me, groups, slots):
    turn, quarter = step // slots, groups // 4
    at_end = (me // quarter) % 3 == 0
    outer = down(groups, 0)
    inner = [
        *down(3 * quarter, quarter), *down(groups, 3 * quarter), *down(quarter, 0)
    ]
    flips = 0
    for at, (far, near) in enumerate(zip(outer, inner)):
        flips = jnp.where(turn == at, jnp.where(at_end, far, near), flips)
    target, bit = 0, 1
    while bit < groups:
        target += (me // bit + flips // bit) % 2 * bit
        bit *= 2
    return target, step % slots


def project_kernel(
    groups, slots, rows_ref, deal_ref, gain_ref, feats_ref, w_ref, keys_ref, values_ref,
    natural, mine, theirs, w_mine, w_give, w_theirs, x_out, x_in, x_scale_out, x_scale_in,
    done, landed, load_sem, w_load_sem, w_give_sem, w_send, w_recv, f_send, f_recv,
    x_send, x_recv, s_send, s_recv, o_send, o_recv, core_sem, x_sem, open_sem,
):
    me = lax.axis_index("gx")
    place = lax.axis_index("gy")
    across = place // 2
    core = place % 2
    other_across, other_core = 1 - across, 1 - core
    core_mate = (me, across * 2 + other_core)
    x_mate = (me, other_across * 2 + core)
    share = w_mine.shape[2]
    total = w_ref.shape[1] // 2
    heads = share // HD
    steps = groups * slots
    leaving = steps - slots

    def columns(block, of_core):
        chip = other_across if block < 2 else across
        first = (block % 2) * total + (chip * 2 + of_core) * share
        return pl.ds(pl.multiple_of(first, 128), share)

    def w_load(b, of_core, into, sem):
        return pltpu.make_async_copy(w_ref.at[:, columns(b, of_core)], into.at[b], sem.at[b])

    loads = [
        pltpu.make_async_copy(
            feats_ref.at[pl.ds(c * groups, groups)], natural[c], load_sem.at[c]
        )
        for c in range(slots)
    ]
    w_loads = [w_load(b, core, w_mine, w_load_sem) for b in range(4)]
    w_gives = [w_load(b, other_core, w_give, w_give_sem) for b in range(4)]
    for copy in (loads[0], w_gives[0], w_gives[1], w_loads[0], *loads[1:], w_loads[1]):
        copy.start()
    for copy in (*w_gives[2:], *w_loads[2:]):
        copy.start()

    barrier = pltpu.get_barrier_semaphore()
    leads = place == 0
    answers = place == 2

    def greet(sem, mate):
        pl.semaphore_signal(sem, inc=1, device_id=mate, device_id_type=MESH)

    @pl.when(core == 0)
    def _():
        greet(barrier, core_mate)
        pl.semaphore_wait(core_sem, 1)

    @pl.when(core == 1)
    def _():
        pl.semaphore_wait(barrier, 1)
        greet(core_sem, core_mate)

    pl.when(leads)(lambda: greet(barrier, x_mate))

    def answer_x():
        pl.semaphore_wait(barrier, 1)
        greet(x_sem, x_mate)
        greet(x_sem, core_mate)

    def meet_x():
        @pl.when(~answers)
        def _():
            pl.semaphore_wait(x_sem, 1)

        @pl.when(leads)
        def _():
            greet(x_sem, core_mate)
            for ahead in range(1, groups):
                greet(barrier, ((me + ahead) % groups, 0))

    def open_deal():
        pl.semaphore_wait(barrier, groups - 1)
        for mate in range(1, 4):
            greet(open_sem, (me, mate))

    w_copies = [
        pltpu.make_async_remote_copy(
            src_ref=w_give.at[b],
            dst_ref=w_theirs.at[b],
            send_sem=w_send.at[b],
            recv_sem=w_recv.at[b],
            device_id=core_mate,
            device_id_type=MESH,
        )
        for b in range(4)
    ]

    def send_weights(b):
        w_gives[b].wait()
        w_copies[b].start()

    def f_copy(k):
        return pltpu.make_async_remote_copy(
            src_ref=mine.at[k], dst_ref=theirs.at[k], send_sem=f_send.at[k],
            recv_sem=f_recv.at[k], device_id=core_mate, device_id_type=MESH,
        )

    def x_copy(b, k):
        return pltpu.make_async_remote_copy(
            src_ref=x_out.at[b, k], dst_ref=x_in.at[b, k], send_sem=x_send.at[b, k],
            recv_sem=x_recv.at[b, k], device_id=x_mate, device_id_type=MESH,
        )

    def s_copy(k):
        return pltpu.make_async_remote_copy(
            src_ref=x_scale_out.at[k], dst_ref=x_scale_in.at[k], send_sem=s_send.at[k],
            recv_sem=s_recv.at[k], device_id=x_mate, device_id_type=MESH,
        )

    def o_copy(b, k, target, landing):
        return pltpu.make_async_remote_copy(
            src_ref=done.at[b, k], dst_ref=landed.at[b, landing], send_sem=o_send.at[b, k],
            recv_sem=o_recv.at[b, landing], device_id=(target, place), device_id_type=MESH,
        )

    def own_column(k):
        target, cls = route(k, me, groups, slots)
        own = 0
        for column in range(groups):
            named = deal_ref[target, cls * groups + column]
            own = jnp.where(named // TPD == me, column, own)
        return own

    def order(k):
        own = own_column(k)
        if isinstance(k, int):
            mine[k] = natural[k % slots][own]
        else:
            for cls in range(slots):

                @pl.when(k % slots == cls)
                def _():
                    mine[k] = natural[cls][own]

        f_copy(k).start()

    send_weights(0)
    loads[0].wait()
    order(0)
    send_weights(1)
    pl.when(answers)(answer_x)
    for copy in loads[1:]:
        copy.wait()
    order(1)
    send_weights(2)
    send_weights(3)
    for k in range(2, AHEAD):
        order(k)
    meet_x()

    def partial(k, block):
        return jnp.dot(
            mine[k], w_mine[block], preferred_element_type=jnp.float32
        ) + jnp.dot(theirs[k], w_theirs[block], preferred_element_type=jnp.float32)

    def weights_here(b):
        w_loads[b].wait()
        w_copies[b].wait_recv()

    def outward(k, first):
        f_copy(k).wait_recv()
        lane = lax.broadcasted_iota(jnp.int32, (TILE, HD), 1)
        peaks = jnp.zeros((TILE, HD), jnp.float32)
        for b in range(2):
            if first:
                weights_here(b)
            sums = partial(k, b)
            for h in range(heads):
                one = sums[:, h * HD : (h + 1) * HD]
                peak = jnp.maximum(jnp.max(jnp.abs(one), axis=-1, keepdims=True), LEAST)
                coded = jnp.round(one * (STEPS / peak)).astype(jnp.int32)
                x_out[b, k, :, h * HD : (h + 1) * HD] = coded.astype(jnp.int16)
                peaks = jnp.where(lane == b * heads + h, peak, peaks)
            if b == 1:
                x_scale_out[k] = jnp.transpose(peaks)[: 2 * heads]
                s_copy(k).start()
            x_copy(b, k).start()

    def finish(k, send):
        target, cls = route(k, me, groups, slots)
        limit = rows_ref[me * TPD + cls * groups + own_column(k)]
        kept = lax.broadcasted_iota(jnp.int32, (TILE, HD), 0) < limit
        for b in range(2):
            part = partial(k, 2 + b)
            if b == 0:
                s_copy(k).wait_recv()
                repeats = HD // (2 * heads)
                peaks = jnp.transpose(jnp.concatenate([x_scale_in[k]] * repeats, axis=0))
            x_copy(b, k).wait_recv()
            for h in range(heads):
                head, at = slice(h * HD, (h + 1) * HD), b * heads + h
                other = x_in[b, k, :, head].astype(jnp.float32)
                one = part[:, head] + other * (peaks[:, at : at + 1] * (1.0 / STEPS))
                if b == 0:
                    mean_square = jnp.mean(one * one, axis=-1, keepdims=True)
                    one = one * lax.rsqrt(mean_square + epsilon) * gain_ref[...]
                done[b, k, :, head] = jnp.where(kept, one, 0.0).astype(jnp.bfloat16)
            if send:
                o_copy(b, k, target, me * slots + cls).start()
            else:
                landed[b, target * slots + cls] = done[b, k]

    def opening(k, carry):
        order(k + AHEAD)
        outward(k, False)
        return carry

    def middle(k, carry):
        @pl.when(k + AHEAD < steps)
        def _():
            order(k + AHEAD)

        @pl.when(~leads & (k == LEAD))
        def _():
            pl.semaphore_wait(open_sem, 1)

        finish(k - LEAD, True)
        outward(k, False)
        return carry

    def closing(k, carry):
        finish(k, True)
        return carry

    outward(0, True)
    order(AHEAD)
    lax.fori_loop(1, LEAD, opening, 0)
    pl.when(leads)(open_deal)
    for b in range(2, 4):
        weights_here(b)
    lax.fori_loop(LEAD, steps, middle, 0)
    lax.fori_loop(steps - LEAD, leaving, closing, 0)
    for copy in w_copies:
        copy.wait_send()

    def sent(k, carry):
        f_copy(k).wait_send()
        s_copy(k).wait_send()
        for b in range(2):
            x_copy(b, k).wait_send()
        return carry

    def dealt(k, carry):
        for b in range(2):
            o_copy(b, k, me, 0).wait_send()
        return carry

    def arrived(ahead, carry):
        source = (me + ahead) % groups
        for cls in range(slots):
            for b in range(2):
                o_copy(b, 0, source, source * slots + cls).wait_recv()
        return carry

    lax.fori_loop(0, leaving, sent, 0)
    for c in range(slots):
        finish(leaving + c, False)
    lax.fori_loop(leaving, steps, sent, 0)
    lax.fori_loop(0, leaving, dealt, 0)
    lax.fori_loop(1, groups, arrived, 0)

    def settle(tile, carry):
        landing = deal_ref[me, tile] // TPD * slots + tile // groups
        rows = pl.ds(pl.multiple_of(tile * TILE, TILE), TILE)
        keys_ref[rows, :] = landed[0, landing]
        values_ref[rows, :] = landed[1, landing]
        return carry

    lax.fori_loop(0, TPD, settle, 0, unroll=16)


def store_kernel(keys_ref, values_ref, keys_out, values_out, sem):
    parts = keys_ref.shape[0] // PARTS
    stores = []
    for which, (source, out) in enumerate(((keys_ref, keys_out), (values_ref, values_out))):
        for part in range(PARTS):
            rows = pl.ds(part * parts, parts)
            stores.append(
                pltpu.make_async_copy(source.at[rows], out.at[rows], sem.at[which, part])
            )
            stores[-1].start()
    for copy in stores:
        copy.wait()


def kernel_local(image_feats, w_kv, k_gain, tile_rows, deal):
    groups = lax.axis_size("gx")
    slots = TPD // groups
    width = image_feats.shape[1]
    share = w_kv.shape[1] // 2 // lax.axis_size("gy")
    steps = TPD
    bf16, f32 = jnp.bfloat16, jnp.float32
    smem = pl.BlockSpec(memory_space=pltpu.SMEM)
    anywhere = pl.BlockSpec(memory_space=pl.ANY)
    dma = pltpu.SemaphoreType.DMA

    tiles = pltpu.VMEM((steps, TILE, width), bf16)
    weights = pltpu.VMEM((4, width, share), bf16)
    codes = pltpu.VMEM((2, steps, TILE, share), jnp.int16)
    scales = pltpu.VMEM((steps, 2 * share // HD, HD), f32)
    results = pltpu.VMEM((2, steps, TILE, share), bf16)
    result = pltpu.VMEM((TPD * TILE, share), bf16)
    vmem = pl.BlockSpec(memory_space=pltpu.VMEM)
    results = pl.pallas_call(
        functools.partial(project_kernel, groups, slots),
        out_shape=(result, result),
        in_specs=[smem, smem, vmem, anywhere, anywhere],
        out_specs=(vmem, vmem),
        scratch_shapes=[
            [pltpu.VMEM((groups, TILE, width), bf16)] * slots, tiles, tiles,
            weights, weights, weights, codes, codes, scales, scales,
            results, results, dma((slots,)), dma((4,)), dma((4,)), dma((4,)), dma((4,)),
            dma((steps,)), dma((steps,)), dma((2, steps)), dma((2, steps)),
            dma((steps,)), dma((steps,)), dma((2, steps)), dma((2, steps)),
            *[pltpu.SemaphoreType.REGULAR] * 3,
        ],
        compiler_params=pltpu.CompilerParams(collective_id=0, has_side_effects=True),
        name="project_and_deal",
    )(tile_rows, deal, k_gain.reshape(1, HD), image_feats.reshape(steps, TILE, width), w_kv)
    stored = jax.ShapeDtypeStruct((TPD * TILE, share), bf16)
    return pl.pallas_call(
        store_kernel,
        out_shape=(stored, stored),
        in_specs=[vmem, vmem],
        out_specs=(anywhere, anywhere),
        scratch_shapes=[dma((2, PARTS))],
        name="store_result",
    )(*[pltpu.with_memory_space_constraint(part, pltpu.VMEM) for part in results])


def solution(mesh):
    groups, width_parts = mesh.shape["gx"], mesh.shape["gy"]
    direct = groups % 4 == 0 and TPD % groups == 0 and width_parts == 4
    local = kernel_local if direct else plain_local
    placed = (P("gx", "gy"), P("gy", None), P(), P(), P())
    return jax.shard_map(
        local, mesh=mesh, in_specs=placed, out_specs=(P("gx", "gy"), P("gx", "gy")), check_vma=False
    )
```
